128 devices in a mesh: grp: 4 (over y_hi, core), ctx: 32 (over z, x, y_lo).
Axes of the slice: x: 4, y: 4 (y_hi: 2, y_lo: 2; y = y_hi * 2 + y_lo), z: 4, core: 2. Of those that a mesh axis runs over, the one named last changes fastest.
Arguments:
- cache: bfloat16 [4, 65536, 576], P('grp', 'ctx'), may hold values from -6 to 6
- queries: bfloat16 [4, 4, 4, 128, 576], P(None, 'grp', None, 'ctx'), may hold values from -72 to 72
- new_latent: bfloat16 [4, 4, 4, 576], P(None, 'grp'), may hold values from -12 to 12
- lengths: int32 [4], replicated, may hold values from 32768 to 65536, as said below
- donor: int32 [4], replicated, may hold values from 0 to 3, as said below
- value_up: bfloat16 [128, 512, 128], P('ctx'), may hold values from -2 to 2
- out_proj: bfloat16 [16384, 7168], P('ctx'), may hold values from -0.09375 to 0.09375
Outputs:
- attn_out: bfloat16 [4, 4, 4, 7168], P(None, 'grp', None, 'ctx')
The draws below stay inside these ranges and needn't reach their ends.
Inputs may be any that keep to these rules, and one draw needn't show every extreme that they name: `lengths`: in every draw some prompt has all 65536 positions valid. `donor`: A slot whose entry is its own index holds a hard prompt; every other entry names such a slot. Slot 3 always holds a hard prompt, and each draw has at least one slot that is not hard.
All inputs are finite; a program needn't handle non-finite values.
Results may differ from the reference program's by a relative error of at most 0.0058.
Values may be sent and summed in bfloat16 or wider, within the bound.
A program may use at most 128 MiB of HBM per device.

```python
import jax
import jax.numpy as jnp
from jax import lax

D = 7168
HEADS = 128
LATENT = 512
VHEAD = 128
CTX_DEV = 2048
SAMPLES = 4
STEPS = 4
HANDOVER = 3
KEYW = 576
GROUPS = 4
CONTEXT = 65536
N_CTX = 32


def draw_cache(key, part):
    drawn_rows = jnp.clip(jax.random.normal(jax.random.fold_in(key, 11), (GROUPS, CONTEXT, KEYW)), -6.0, 6.0)
    return drawn_rows.astype(jnp.bfloat16)


def draw_queries(key, part):
    draw_shape = (STEPS, GROUPS, SAMPLES, HEADS, KEYW)
    drawn_rows = jnp.clip(1.5 * jax.random.normal(jax.random.fold_in(key, 12), draw_shape), -6.0, 6.0)
    return drawn_rows.astype(jnp.bfloat16)


def draw_lengths(key, part):
    spread = jax.random.randint(jax.random.fold_in(key, 21), (GROUPS,), CONTEXT // 2, CONTEXT + 1)
    full_group = jax.random.randint(jax.random.fold_in(key, 22), (), 0, GROUPS)
    return jnp.where(jnp.arange(GROUPS) == full_group, CONTEXT, spread).astype(jnp.int32)


def draw_donor(key, part):
    rest_order = jax.random.permutation(jax.random.fold_in(key, 31), GROUPS - 1).astype(jnp.int32)
    shuffled = jnp.concatenate([jnp.full((1,), GROUPS - 1, jnp.int32), rest_order])
    hard_count = jax.random.randint(jax.random.fold_in(key, 32), (), 1, GROUPS)
    position = jnp.argsort(shuffled, stable=True)
    chosen = jax.random.randint(jax.random.fold_in(key, 33), (GROUPS,), 0, hard_count)
    return jnp.where(position < hard_count, jnp.arange(GROUPS), shuffled[chosen]).astype(jnp.int32)


def raised(result, rng, source, target, blocks, factor):
    def block_of(axis_at):
        return (jnp.arange(result.shape[axis_at]) // (result.shape[axis_at] // blocks)).reshape((-1,) + (1,) * (result.ndim - 1 - axis_at))

    one_side = jax.random.permutation(rng, blocks)[block_of(target)]
    second = (block_of(target) + blocks // 2) % blocks
    return jnp.where((block_of(source) == one_side) | (block_of(source) == second), factor * result, result)


def levels(key, dims, split, smallest, largest):
    def one(axis_at, shards_of):
        steps = jax.random.uniform(jax.random.fold_in(jax.random.fold_in(key, 6), axis_at), (shards_of,), jnp.float32, smallest / len(split), largest / len(split))
        return jnp.repeat(jnp.exp(steps), dims[axis_at] // shards_of).reshape((-1,) + (1,) * (len(dims) - axis_at - 1))

    level = one(*split[0])
    for cut in split[1:]:
        level = level * one(*cut)
    return level


def scatter_about(rng, shape, scale, bound, pieces=(), kind=jnp.bfloat16):
    gain = levels(rng, shape, pieces, -0.22, 0.18) if pieces else 1.0
    entries = jax.random.normal(rng, shape, jnp.float32) * scale * gain
    return jnp.minimum(jnp.maximum(entries, -bound), bound).astype(kind)


def noise_with(stream_key, shape, deviation, most, pieces, heavy, held_as=jnp.bfloat16):
    values = deviation * jax.random.normal(stream_key, shape, jnp.float32)
    if pieces:
        values = values * levels(stream_key, shape, pieces, -0.22, 0.18)
    return jnp.clip(raised(values, jax.random.fold_in(stream_key, 3), *heavy), -most, most).astype(held_as)


def setup_inputs(seed: int = 0) -> dict:
    arg_keys = jax.random.split(jax.random.key(seed), 8)
    return {
        "cache": draw_cache(jax.random.fold_in(arg_keys[7], 71), 0),
        "queries": draw_queries(jax.random.fold_in(arg_keys[7], 71), 0),
        "new_latent": scatter_about(arg_keys[2], (STEPS, GROUPS, SAMPLES, KEYW), 2.0, 12.0, ((1, 4),)),
        "lengths": draw_lengths(jax.random.fold_in(arg_keys[7], 71), 0),
        "donor": draw_donor(jax.random.fold_in(arg_keys[7], 71), 0),
        "value_up": scatter_about(arg_keys[5], (HEADS, LATENT, VHEAD), 0.35, 2.0, ((0, 32),)),
        "out_proj": noise_with(arg_keys[6], (HEADS * VHEAD, D), (HEADS * VHEAD) ** -0.5, 0.09375, ((0, 32),), (0, 1, 32, 2.75)),
    }


score_scale = 192.0 ** -0.5
far_below = -1e30


def block_partial(query_rows, cache_rows, valid_mask):
    logits = jnp.dot(query_rows, cache_rows.T, preferred_element_type=jnp.float32) * score_scale
    logits = jnp.where(valid_mask[None, :], logits, far_below)
    top_score = jnp.max(logits, axis=1)
    weights = jnp.where(valid_mask[None, :], jnp.exp(logits - top_score[:, None]), 0.0)
    weight_sum = jnp.sum(weights, axis=1)
    partial_out = jnp.dot(weights.astype(jnp.bfloat16), cache_rows[:, :LATENT], preferred_element_type=jnp.float32)
    return top_score, weight_sum, partial_out


def combine(earlier, later):
    top_score = jnp.maximum(earlier[0], later[0])
    scale_one = jnp.exp(earlier[0] - top_score)
    scale_two = jnp.exp(later[0] - top_score)
    return (top_score, earlier[1] * scale_one + later[1] * scale_two,
            earlier[2] * scale_one[..., None] + later[2] * scale_two[..., None])


def reference(cache, queries, new_latent, lengths, donor, value_up, out_proj):
    row_count = SAMPLES * HEADS
    highest = lax.Precision.HIGHEST
    step_outs = []
    for step_index in range(STEPS):
        group_outs = []
        for group_index in range(GROUPS):
            if step_index < HANDOVER:
                prompt_rows = cache[group_index]
                prompt_len = lengths[group_index]
            else:
                prompt_rows = lax.dynamic_index_in_dim(cache, donor[group_index], 0, keepdims=False)
                prompt_len = lax.dynamic_index_in_dim(lengths, donor[group_index], 0, keepdims=False)
            query_rows = queries[step_index, group_index].reshape(row_count, KEYW)

            def visit(carried, block_no):
                offset_at = (block_no * CTX_DEV).astype(jnp.int32)
                cache_block = lax.dynamic_slice_in_dim(prompt_rows, offset_at, CTX_DEV, 0)
                valid_mask = offset_at + jnp.arange(CTX_DEV, dtype=jnp.int32) < prompt_len
                return combine(carried, block_partial(query_rows, cache_block, valid_mask)), None

            initial = (jnp.full((row_count,), far_below, jnp.float32), jnp.zeros((row_count,), jnp.float32),
                       jnp.zeros((row_count, LATENT), jnp.float32))
            merged, _ = lax.scan(visit, initial, jnp.arange(N_CTX, dtype=jnp.int32))
            merged = (merged[0].reshape(SAMPLES, HEADS), merged[1].reshape(SAMPLES, HEADS),
                      merged[2].reshape(SAMPLES, HEADS, LATENT))
            fresh_keys = new_latent[:step_index + 1, group_index].astype(jnp.float32)
            query_wide = queries[step_index, group_index].astype(jnp.float32)
            fresh_logits = jnp.einsum('shc,tsc->sht', query_wide, fresh_keys, precision=highest) * score_scale
            fresh_top = jnp.max(fresh_logits, axis=2)
            fresh_weights = jnp.exp(fresh_logits - fresh_top[..., None])
            fresh_sum = jnp.sum(fresh_weights, axis=2)
            fresh_part = jnp.einsum('sht,tsl->shl', fresh_weights, fresh_keys[..., :LATENT], precision=highest)
            merged = combine(merged, (fresh_top, fresh_sum, fresh_part))
            attended = (merged[2] / merged[1][..., None]).astype(jnp.bfloat16)
            head_values = jnp.einsum('shl,hlv->shv', attended.astype(jnp.float32), value_up.astype(jnp.float32),
                                     precision=highest).astype(jnp.bfloat16)
            mixed_out = jnp.dot(head_values.reshape(SAMPLES, HEADS * VHEAD), out_proj,
                                preferred_element_type=jnp.float32).astype(jnp.bfloat16)
            group_outs.append(mixed_out)
        step_outs.append(jnp.stack(group_outs))
    return jnp.stack(step_outs)
```

```python
import functools

import jax
import jax.numpy as jnp
from jax import lax
from jax.experimental import pallas as pl
from jax.experimental.pallas import tpu as pltpu
from jax.sharding import PartitionSpec as P

MESH = pl.DeviceIdType.MESH
LATENT = 512
KEYW = 576
CTX = 2048
ROWS = 16
UNIT = 256
NPART = 5
OUTW = 224
NPEER = 32
SCALE2 = (192.0 ** -0.5) * 1.4426950408889634
LOW = -1e30
FLOOR = -1e29
BF = jnp.bfloat16
F32 = jnp.float32


def rounded(v):
    return v.astype(BF).astype(F32)


def lanes_of(shape):
    return lax.broadcasted_iota(jnp.int32, shape, 1)


def put(tile, lane, j, m, s):
    hi = rounded(s)
    tile = jnp.where(lane == j, m, tile)
    tile = jnp.where(lane == 16 + j, hi, tile)
    return jnp.where(lane == 32 + j, s - hi, tile)


def take(tile, j):
    return tile[:, j:j + 1], tile[:, 16 + j:17 + j] + tile[:, 32 + j:33 + j]


def merged(ma, sa, oa, mb, sb, ob):
    top = jnp.maximum(ma, mb)
    fa = jnp.exp2(ma - top)
    fb = jnp.exp2(mb - top)
    return top, sa * fa + sb * fb, oa * fa + ob * fb


def kernel(lim_ref, sel_ref, q_ref, nl_ref, cache_ref, vu_ref, op_ref, out_ref,
           cbuf, qbuf, obuf, stat, ra, ras, rc, rcs, rb, rbs, rd, rds, ry, rys, rf, rfs,
           sbuf, rbuf, opv, vuv, scr, fo, fm, fs,
           csem, gsend, grecv, rsend, rrecv, xsend, xrecv, ysend, yrecv):
    g = lax.axis_index("grp")
    c = lax.axis_index("ctx")
    h = g // 2
    k = g % 2
    z = c // 8
    x = (c // 2) % 4
    y = c % 2
    other = c + 1 - 2 * y

    def nbr(p, axis_b, delta):
        along_z = (p == 0) != axis_b
        if along_z:
            return (g, ((z + delta + 4) % 4) * 8 + x * 2 + y)
        return (g, z * 8 + ((x + delta + 4) % 4) * 2 + y)

    def rdma(src, dst, ss, rs, dev):
        return pltpu.make_async_remote_copy(src_ref=src, dst_ref=dst, send_sem=ss, recv_sem=rs,
                                            device_id=dev, device_id_type=MESH)

    barrier = pltpu.get_barrier_semaphore()

    def greet(i, carry):
        pl.semaphore_signal(barrier, inc=1, device_id=(g, (c + i) % NPEER), device_id_type=MESH)
        return carry

    lax.fori_loop(1, NPEER, greet, 0)
    for dg in range(1, 4):
        for dc in (c, other):
            pl.semaphore_signal(barrier, inc=1, device_id=((g + dg) % 4, dc), device_id_type=MESH)

    own_copy = pltpu.make_async_copy(cache_ref, cbuf.at[0], csem.at[0])
    own_copy.start()
    op_copy = pltpu.make_async_copy(op_ref, opv, csem.at[1])
    op_copy.start()
    vu_copy = pltpu.make_async_copy(vu_ref, vuv, csem.at[2])
    vu_copy.start()
    for t in range(3):
        qbuf[0, t, 0, 0] = q_ref[t]

    pl.semaphore_wait(barrier, NPEER - 1 + 6)

    def ycopy(t):
        return rdma(q_ref.at[t], qbuf.at[1, t, 0, 0], gsend.at[t], grecv.at[t], (g, other))

    for t in range(3):
        ycopy(t).start()

    def slot_copy(s, i, dev):
        return rdma(q_ref.at[3], qbuf.at[s % 2, 3 + s // 2, 0, 0], gsend.at[3 + i], grecv.at[3 + s], dev)

    for hh in range(2):
        for yy in range(2):
            dev = (2 * hh + y, z * 8 + x * 2 + yy)
            mine = (2 * hh + y == g) & (y == yy)

            @pl.when(jnp.logical_not(mine))
            def _():
                slot_copy(g, 2 * hh + yy, dev).start()

    @pl.when(y == k)
    def _():
        qbuf[g % 2, 3 + g // 2, 0, 0] = q_ref[3]

    swap = rdma(cache_ref, cbuf.at[1], csem.at[3], csem.at[4], (g + 1 - 2 * k, c))
    swap.start()

    lane_k = lax.broadcasted_iota(jnp.int32, (ROWS, ROWS), 1)
    row_s = lax.broadcasted_iota(jnp.int32, (ROWS, ROWS), 0) // 4
    nl = nl_ref[...]
    for t in range(4):
        logits = lax.dot_general(q_ref[t], nl, (((1,), (1,)), ((), ())), preferred_element_type=F32)
        ok = (lane_k % 4 == row_s) & (lane_k // 4 <= t)
        logits = jnp.where(ok, logits * SCALE2, LOW)
        top = jnp.max(logits, axis=1, keepdims=True)
        w = jnp.where(ok, jnp.exp2(logits - top), 0.0)
        whi = w.astype(BF)
        wlo = (w - whi.astype(F32)).astype(BF)
        val = nl[:, :LATENT]
        fo[t] = (jnp.dot(whi, val, preferred_element_type=F32)
                 + jnp.dot(wlo, val, preferred_element_type=F32))
        fm[t] = jnp.broadcast_to(top, (ROWS, 128))
        fs[t] = jnp.broadcast_to(jnp.sum(w, axis=1, keepdims=True), (ROWS, 128))

    def sems(p, t, i):
        n = (p * NPART + t) * 8 + i
        return gsend.at[8 + n], grecv.at[8 + n]

    def g1(p, t, sign):
        return rdma(qbuf.at[p, t, 0, 0], qbuf.at[p, t, 0, 3 if sign > 0 else 1],
                    *sems(p, t, 0 if sign > 0 else 1), nbr(p, True, sign))

    def g1f(p, t):
        sign = 1 if t % 2 == 0 else -1
        return rdma(qbuf.at[p, t, 0, 3 if sign > 0 else 1], qbuf.at[p, t, 0, 2],
                    *sems(p, t, 2), nbr(p, True, sign))

    def g2(p, t, sign):
        return rdma(qbuf.at[p, t, 0], qbuf.at[p, t, 3 if sign > 0 else 1],
                    *sems(p, t, 3 if sign > 0 else 4), nbr(p, False, sign))

    def g2f(p, t, sign):
        half = pl.ds(0, 2) if sign > 0 else pl.ds(2, 2)
        return rdma(qbuf.at[p, t, 3 if sign > 0 else 1, half], qbuf.at[p, t, 2, half],
                    *sems(p, t, 5 if sign > 0 else 6), nbr(p, False, sign))

    units = [(p, t) for t in range(NPART) for p in range(2)]
    for p, t in units:
        if t < 3:
            if p == 1:
                ycopy(t).wait_recv()
        else:
            s = (t - 3) * 2 + p
            mine = (g == s) & (y == k)

            @pl.when(jnp.logical_not(mine))
            def _():
                slot_copy(s, 0, (g, c)).wait_recv()
        g1(p, t, 1).start()
        g1(p, t, -1).start()
    for p, t in units:
        first, second = (1, -1) if t % 2 == 0 else (-1, 1)
        g1(p, t, first).wait_recv()
        g1f(p, t).start()
    for p, t in units:
        second = -1 if t % 2 == 0 else 1
        g1(p, t, second).wait_recv()
        g1f(p, t).wait_recv()
        g2(p, t, 1).start()
        g2(p, t, -1).start()
    for p, t in units:
        for sign in (1, -1):
            g2(p, t, sign).wait_recv()
            g2f(p, t, sign).start()
    for p, t in units:
        for sign in (1, -1):
            g2f(p, t, sign).wait_recv()

    own_copy.wait()
    swap.wait()

    lane = lanes_of((ROWS, 128))
    nj = 4
    wj = CTX // nj

    def attend(u, carry):
        p = u % 2
        t = u // 2
        limit = lim_ref[u]
        sel = sel_ref[u]
        q = qbuf[p, t].reshape(UNIT, KEYW)
        top = jnp.full((UNIT, 1), FLOOR, F32)
        for j in range(nj):
            pos = lax.broadcasted_iota(jnp.int32, (1, wj), 1) + j * wj
            bias = jnp.where(pos < limit, 0.0, LOW)
            sc = jnp.dot(q, cbuf[sel, :, j * wj:(j + 1) * wj], preferred_element_type=F32) * SCALE2 + bias
            scr[:, j * wj:(j + 1) * wj] = sc
            top = jnp.maximum(top, jnp.max(sc, axis=1, keepdims=True))
        top = rounded(top)
        total = jnp.zeros((UNIT, 1), F32)
        acc = jnp.zeros((UNIT, LATENT), F32)
        for j in range(nj):
            w = jnp.exp2(scr[:, j * wj:(j + 1) * wj] - top)
            total = total + jnp.sum(w, axis=1, keepdims=True)
            acc = acc + lax.dot_general(w.astype(BF), cbuf[sel, :LATENT, j * wj:(j + 1) * wj],
                                        (((1,), (1,)), ((), ())), preferred_element_type=F32)
        obuf[p, t] = acc.astype(BF).reshape(4, 4, ROWS, LATENT)
        tile = jnp.zeros((ROWS, 128), F32)
        for j in range(16):
            tile = put(tile, lane, j, top[j * ROWS:(j + 1) * ROWS], total[j * ROWS:(j + 1) * ROWS])
        stat[p, t] = tile.astype(BF)
        return carry

    lax.fori_loop(0, 2 * NPART, attend, 0)

    def rsem(p, t, i):
        n = (p * NPART + t) * 16 + i
        return rsend.at[n], rrecv.at[n]

    def fold(p, t, a, b, tile_in, j_in, data_in, tile):
        j = a * 4 + b
        ma, sa = take(tile, j)
        mb, sb = take(tile_in, j_in)
        m, s, o = merged(ma, sa, obuf[p, t, a, b].astype(F32), mb, sb, data_in.astype(F32))
        obuf[p, t, a, b] = o.astype(BF)
        return put(tile, lane, j, m, s)

    def a1(p, t, sign):
        i = 0 if sign > 0 else 1
        half = pl.ds(0, 2) if sign > 0 else pl.ds(2, 2)
        dev = nbr(p, False, sign)
        return (rdma(obuf.at[p, t, 2, half], ra.at[p, t, i], *rsem(p, t, i), dev),
                rdma(stat.at[p, t], ras.at[p, t, i], *rsem(p, t, 2 + i), dev))

    def a2(p, t, sign):
        i = 0 if sign > 0 else 1
        dev = nbr(p, False, sign)
        return (rdma(obuf.at[p, t, 1 if sign > 0 else 3], rc.at[p, t, i], *rsem(p, t, 4 + i), dev),
                rdma(stat.at[p, t], rcs.at[p, t, i], *rsem(p, t, 6 + i), dev))

    def b1(p, t):
        sign = 1 if t % 2 == 0 else -1
        dev = nbr(p, True, sign)
        return (rdma(obuf.at[p, t, 0, 2], rb.at[p, t], *rsem(p, t, 8), dev),
                rdma(stat.at[p, t], rbs.at[p, t], *rsem(p, t, 9), dev))

    def b2(p, t, sign):
        i = 0 if sign > 0 else 1
        dev = nbr(p, True, sign)
        return (rdma(obuf.at[p, t, 0, 1 if sign > 0 else 3], rd.at[p, t, i], *rsem(p, t, 10 + i), dev),
                rdma(stat.at[p, t], rds.at[p, t, i], *rsem(p, t, 12 + i), dev))

    def start(pair):
        for cp in pair:
            cp.start()

    def got(pair):
        for cp in pair:
            cp.wait_recv()

    def gone(pair):
        for cp in pair:
            cp.wait_send()

    for p, t in units:
        start(a1(p, t, 1))
        start(a1(p, t, -1))
    for p, t in units:
        for sign in (1, -1):
            got(a1(p, t, sign))
            gone(a1(p, t, sign))
        tile = stat[p, t].astype(F32)
        for i in range(2):
            tin = ras[p, t, i].astype(F32)
            for b in range(2):
                bb = 2 * i + b
                tile = fold(p, t, 1 if i == 0 else 3, bb, tin, 8 + bb, ra[p, t, i, b], tile)
        stat[p, t] = tile.astype(BF)
        start(a2(p, t, 1))
        start(a2(p, t, -1))
    for p, t in units:
        for sign in (1, -1):
            got(a2(p, t, sign))
            gone(a2(p, t, sign))
        tile = stat[p, t].astype(F32)
        for i in range(2):
            tin = rcs[p, t, i].astype(F32)
            for b in range(4):
                tile = fold(p, t, 0, b, tin, (4 if i == 0 else 12) + b, rc[p, t, i, b], tile)
        stat[p, t] = tile.astype(BF)
        start(b1(p, t))
    for p, t in units:
        got(b1(p, t))
        gone(b1(p, t))
        tile = stat[p, t].astype(F32)
        tile = fold(p, t, 0, 1 if t % 2 == 0 else 3, rbs[p, t].astype(F32), 2, rb[p, t], tile)
        stat[p, t] = tile.astype(BF)
        start(b2(p, t, 1))
        start(b2(p, t, -1))

    def yback(t):
        return (rdma(obuf.at[1, t, 0, 0], ry.at[t], ysend.at[2 * t], yrecv.at[2 * t], (g, other)),
                rdma(stat.at[1, t], rys.at[t], ysend.at[2 * t + 1], yrecv.at[2 * t + 1], (g, other)))

    def sback(s, src):
        dev = (s, z * 8 + x * 2 + k)
        return (rdma(obuf.at[s % 2, 3 + s // 2, 0, 0], rf.at[src], ysend.at[6 + 2 * s], yrecv.at[6 + 2 * src], dev),
                rdma(stat.at[s % 2, 3 + s // 2], rfs.at[src], ysend.at[7 + 2 * s], yrecv.at[7 + 2 * src], dev))

    for p, t in units:
        for sign in (1, -1):
            got(b2(p, t, sign))
            gone(b2(p, t, sign))
        tile = stat[p, t].astype(F32)
        for i in range(2):
            tile = fold(p, t, 0, 0, rds[p, t, i].astype(F32), 1 if i == 0 else 3, rd[p, t, i], tile)
        stat[p, t] = tile.astype(BF)
        if t < 3:
            if p == 1:
                start(yback(t))
        else:
            s = (t - 3) * 2 + p
            mine = (g == s) & (y == k)

            @pl.when(jnp.logical_not(mine))
            def _():
                start(sback(s, 2 * h + y))

            @pl.when(mine)
            def _():
                rf[2 * h + y] = obuf[p, t, 0, 0]
                rfs[2 * h + y] = stat[p, t]

    att = []

    def finish(t, m, s, o):
        m, s, o = merged(m, s, o, fm[t][:, :1], fs[t][:, :1], fo[t])
        att.append((o / s).astype(BF))

    for t in range(3):
        got(yback(t))
        m, s = take(stat[0, t].astype(F32), 0)
        mb, sb = take(rys[t].astype(F32), 0)
        m, s, o = merged(m, s, obuf[0, t, 0, 0].astype(F32), mb, sb, ry[t].astype(F32))
        finish(t, m, s, o)
    m = s = o = None
    for src in range(4):
        mine = (y == k) & (src == 2 * h + y)

        @pl.when(jnp.logical_not(mine))
        def _():
            got(sback(0, src))
        mb, sb = take(rfs[src].astype(F32), 0)
        ob = rf[src].astype(F32)
        if src == 0:
            m, s, o = mb, sb, ob
        else:
            m, s, o = merged(m, s, o, mb, sb, ob)
    finish(3, m, s, o)

    attended = jnp.concatenate(att, axis=0)
    vu_copy.wait()
    op_copy.wait()
    row_head = lax.broadcasted_iota(jnp.int32, (64, 128), 0) % 4
    pieces = []
    for head in range(4):
        hv = jnp.dot(attended, vuv[head], preferred_element_type=F32)
        pieces.append(jnp.where(row_head == head, hv, 0.0).astype(BF))
    spread = jnp.concatenate(pieces, axis=1)
    pick = (lax.broadcasted_iota(jnp.int32, (ROWS, 64), 1) // 4
            == lax.broadcasted_iota(jnp.int32, (ROWS, 64), 0))
    joined = jnp.dot(jnp.where(pick, 1.0, 0.0).astype(BF), spread, preferred_element_type=F32).astype(BF)

    def outc(dest, rel):
        return rdma(sbuf.at[dest], rbuf.at[rel], xsend.at[dest], xrecv.at[rel], (g, dest))

    width = 8 * OUTW
    for blk in range(4):
        term = jnp.dot(joined, opv[:, blk * width:(blk + 1) * width], preferred_element_type=F32)
        for i in range(8):
            sbuf[blk * 8 + i, :, :OUTW] = term[:, i * OUTW:(i + 1) * OUTW].astype(BF)

    def send_out(i, carry):
        outc((c + i) % NPEER, (NPEER - i) % NPEER).start()
        return carry

    lax.fori_loop(1, NPEER, send_out, 0)

    for t in range(3):
        ycopy(t).wait_send()
        gone(yback(t))
    for hh in range(2):
        for yy in range(2):
            mine = (2 * hh + y == g) & (y == yy)

            @pl.when(jnp.logical_not(mine))
            def _():
                slot_copy(g, 2 * hh + yy, (g, c)).wait_send()
    for s in range(4):
        mine = (g == s) & (y == k)

        @pl.when(jnp.logical_not(mine))
        def _():
            gone(sback(s, 0))
    for p, t in units:
        g1f(p, t).wait_send()
        for sign in (1, -1):
            g1(p, t, sign).wait_send()
            g2(p, t, sign).wait_send()
            g2f(p, t, sign).wait_send()

    res = sbuf[c][:, :OUTW].astype(F32)
    for rel in range(1, NPEER):
        pltpu.make_async_remote_copy(src_ref=sbuf.at[0], dst_ref=rbuf.at[rel], send_sem=xsend.at[0],
                                     recv_sem=xrecv.at[rel], device_id=(g, c), device_id_type=MESH).wait_recv()
        res = res + rbuf[rel][:, :OUTW].astype(F32)
    out_ref[...] = res.astype(BF)

    def sent_out(i, carry):
        outc((c + i) % NPEER, (NPEER - i) % NPEER).wait_send()
        return carry

    lax.fori_loop(1, NPEER, sent_out, 0)


def body(cache, queries, new_latent, lengths, donor, value_up, out_proj):
    g = lax.axis_index("grp")
    c = lax.axis_index("ctx")
    start = c * CTX
    own = jnp.sum(jnp.where(jnp.arange(4, dtype=jnp.int32) == g, lengths, 0)) - start
    src_len = jnp.sum(jnp.where(donor[:, None] == jnp.arange(4, dtype=jnp.int32)[None], lengths[None], 0), axis=1)
    slot_lim = jnp.where(donor // 2 == g // 2, src_len - start, 0)
    slot_sel = (donor % 2 != g % 2).astype(jnp.int32)
    limits = jnp.concatenate([jnp.broadcast_to(own, (6,)), slot_lim]).astype(jnp.int32)
    select = jnp.concatenate([jnp.zeros((6,), jnp.int32), slot_sel])
    keys = jnp.swapaxes(cache[0], 0, 1)
    q = queries.reshape(4, ROWS, KEYW)
    nl = new_latent.reshape(ROWS, KEYW)
    VM, SM, ANY = pltpu.VMEM, pltpu.SMEM, pl.ANY
    U = (2, NPART)
    dma = pltpu.SemaphoreType.DMA
    out = pl.pallas_call(
        kernel,
        out_shape=jax.ShapeDtypeStruct((ROWS, OUTW), BF),
        in_specs=[pl.BlockSpec(memory_space=m) for m in (SM, SM, VM, VM, ANY, ANY, ANY)],
        out_specs=pl.BlockSpec(memory_space=VM),
        scratch_shapes=[
            VM((2, KEYW, CTX), BF),
            VM(U + (4, 4, ROWS, KEYW), BF),
            VM(U + (4, 4, ROWS, LATENT), BF),
            VM(U + (ROWS, 128), BF),
            VM(U + (2, 2, ROWS, LATENT), BF), VM(U + (2, ROWS, 128), BF),
            VM(U + (2, 4, ROWS, LATENT), BF), VM(U + (2, ROWS, 128), BF),
            VM(U + (ROWS, LATENT), BF), VM(U + (ROWS, 128), BF),
            VM(U + (2, ROWS, LATENT), BF), VM(U + (2, ROWS, 128), BF),
            VM((3, ROWS, LATENT), BF), VM((3, ROWS, 128), BF),
            VM((4, ROWS, LATENT), BF), VM((4, ROWS, 128), BF),
            VM((NPEER, ROWS, 256), BF), VM((NPEER, ROWS, 256), BF),
            VM((512, 7168), BF), VM((4, LATENT, 128), BF),
            VM((UNIT, CTX), F32),
            VM((4, ROWS, LATENT), F32), VM((4, ROWS, 128), F32), VM((4, ROWS, 128), F32),
            dma((5,)), dma((88,)), dma((88,)), dma((160,)), dma((160,)),
            dma((NPEER,)), dma((NPEER,)), dma((16,)), dma((16,)),
        ],
        compiler_params=pltpu.CompilerParams(collective_id=0, has_side_effects=True,
                                             vmem_limit_bytes=56 * 1024 * 1024),
        name="mla_step",
    )(limits, select, q, nl, keys, value_up, out_proj)
    return out.reshape(4, 1, 4, OUTW)


def solution(mesh):
    return jax.shard_map(
        body,
        mesh=mesh,
        in_specs=(
            P("grp", "ctx", None),
            P(None, "grp", None, "ctx", None),
            P(None, "grp", None, None),
            P(),
            P(),
            P("ctx", None, None),
            P("ctx", None),
        ),
        out_specs=P(None, "grp", None, "ctx"),
        check_vma=False,
    )
```

```python
import functools

import jax
import jax.numpy as jnp
from jax import lax
from jax.experimental import pallas as pl
from jax.experimental.pallas import tpu as pltpu
from jax.sharding import PartitionSpec as P

MESH = pl.DeviceIdType.MESH
LATENT = 512
KEYW = 576
CTX = 2048
ROWS = 16
UNIT = 256
NPART = 5
OUTW = 224
NPEER = 32
SCALE2 = (192.0 ** -0.5) * 1.4426950408889634
LOW = -1e30
FLOOR = -1e29
BF = jnp.bfloat16
F32 = jnp.float32


def rounded(v):
    return v.astype(BF).astype(F32)


def lanes_of(shape):
    return lax.broadcasted_iota(jnp.int32, shape, 1)


def stats(tile):
    t = tile.astype(F32)
    return t, pltpu.roll(t, 124, 1) + pltpu.roll(t, 120, 1)


def combine(parts):
    top = parts[0][0]
    for t, _ in parts[1:]:
        top = jnp.maximum(top, t)
    factors = [jnp.exp2(t - top) for t, _ in parts]
    total = factors[0] * parts[0][1]
    for f, (_, v) in zip(factors[1:], parts[1:]):
        total = total + f * v
    return top, total, factors


def packed(top, total):
    lane = lanes_of(top.shape)
    hi = rounded(total)
    lo = total - hi
    return jnp.where(lane < 4, top, jnp.where(lane < 8, pltpu.roll(hi, 4, 1), pltpu.roll(lo, 8, 1))).astype(BF)


def kernel(len_ref, don_ref, q_ref, nl_ref, cache_ref, vu_ref, op_ref, out_ref,
           cbuf, qown, qbuf, obuf, stat, ra, ras, rc, rcs, rd, rds, rf, rfs,
           sbuf, rbuf, opv, vuv, scr, fo, fst,
           csem, hsend, hrecv, gsend, grecv, rsend, rrecv, xsend, xrecv, dsend, drecv, fsend, frecv):
    g = lax.axis_index("grp")
    c = lax.axis_index("ctx")
    h = g // 2
    k = g % 2
    z = c // 8
    x = (c // 2) % 4
    y = c % 2
    other = c + 1 - 2 * y

    def at(dz, dx, yy):
        return ((z + dz + 4) % 4) * 8 + ((x + dx + 4) % 4) * 2 + yy

    def nbr(p, axis_b, delta):
        return (g, at(delta, 0, y) if (p == 0) != axis_b else at(0, delta, y))

    def rdma(src, dst, ss, rs, dev):
        return pltpu.make_async_remote_copy(src_ref=src, dst_ref=dst, send_sem=ss, recv_sem=rs,
                                            device_id=dev, device_id_type=MESH)

    scope = [None]

    def phase(name):
        if scope[0] is not None:
            scope[0].__exit__(None, None, None)
            scope[0] = None
        if name:
            scope[0] = jax.named_scope(name)
            scope[0].__enter__()

    phase("enter")
    barrier = pltpu.get_barrier_semaphore()

    def greet(i, carry):
        pl.semaphore_signal(barrier, inc=1, device_id=(g, (c + i) % NPEER), device_id_type=MESH)
        return carry

    lax.fori_loop(1, NPEER, greet, 0)
    places = [(0, 0)] + [(d, 0) for d in range(1, 4)] + [(0, d) for d in range(1, 4)]
    for dg in range(1, 4):
        for dz, dx in places:
            for yy in range(2):
                pl.semaphore_signal(barrier, inc=1, device_id=((g + dg) % 4, at(dz, dx, yy)), device_id_type=MESH)

    own_copy = pltpu.make_async_copy(cache_ref, cbuf.at[0], csem.at[0])
    own_copy.start()
    vu_copy = pltpu.make_async_copy(vu_ref, vuv, csem.at[2])
    vu_copy.start()
    op_copy = pltpu.make_async_copy(op_ref, opv, csem.at[1])
    op_copy.start()
    for t in range(4):
        for s in range(4):
            qown[t, 4 * s:4 * s + 4] = q_ref[t, 0, s]
    for t in range(3):
        qbuf[0, t, 0, 0] = qown[t]

    lane = lanes_of((ROWS, 128))
    lane_k = lanes_of((ROWS, 4))
    row_s = lax.broadcasted_iota(jnp.int32, (ROWS, 4), 0) // 4
    for t in range(4):
        q = qown[t]
        logits = []
        for u in range(t + 1):
            lg = lax.dot_general(q, nl_ref[u, 0], (((1,), (1,)), ((), ())), preferred_element_type=F32)
            logits.append(jnp.where(lane_k == row_s, lg * SCALE2, LOW))
        top = jnp.max(logits[0], axis=1, keepdims=True)
        for lg in logits[1:]:
            top = jnp.maximum(top, jnp.max(lg, axis=1, keepdims=True))
        total = jnp.zeros((ROWS, 1), F32)
        acc = jnp.zeros((ROWS, LATENT), F32)
        for u in range(t + 1):
            w = jnp.where(lane_k == row_s, jnp.exp2(logits[u] - top), 0.0)
            total = total + jnp.sum(w, axis=1, keepdims=True)
            val = nl_ref[u, 0][:, :LATENT]
            whi = w.astype(BF)
            wlo = (w - whi.astype(F32)).astype(BF)
            acc = acc + (jnp.dot(whi, val, preferred_element_type=F32)
                         + jnp.dot(wlo, val, preferred_element_type=F32))
        fo[t] = acc
        fst[t, 0] = jnp.broadcast_to(top, (ROWS, 128))
        fst[t, 1] = jnp.broadcast_to(total, (ROWS, 128))

    pl.semaphore_wait(barrier, NPEER - 1 + 42)
    phase("prep")

    def hsems(p, t, d):
        n = (p * NPART + t) * 4 + d
        return hsend.at[n], hrecv.at[n]

    def h0(t, d):
        return rdma(qown.at[t], qbuf.at[0, t, 0, (4 - d) % 4], *hsems(0, t, d), (g, at(0, d, y)))

    def h1(t, d):
        return rdma(qown.at[t], qbuf.at[1, t, 0, (4 - d) % 4], *hsems(1, t, d), (g, at(d, 0, 1 - y)))

    def hs(hh, yy, d):
        p = g % 2
        t = 3 + g // 2
        dz = jnp.where(p == 0, 0, d)
        dev = (2 * hh + y, at(dz, d - dz, yy))
        n = (p * NPART + t) * 4 + d
        return rdma(qown.at[3], qbuf.at[p, t, 0, (4 - d) % 4],
                    hsend.at[40 + (2 * hh + yy) * 4 + d], hrecv.at[n], dev)

    def sems(p, t, i):
        n = (p * NPART + t) * 4 + i
        return gsend.at[n], grecv.at[n]

    def fwd_sign(p, t):
        return 1 if (t + p) % 2 == 0 else -1

    def g2(p, t, sign):
        return rdma(qbuf.at[p, t, 0], qbuf.at[p, t, 3 if sign > 0 else 1],
                    *sems(p, t, 0 if sign > 0 else 1), nbr(p, False, sign))

    def g2f(p, t, sign):
        half = pl.ds(0, 2) if sign > 0 else pl.ds(2, 2)
        return rdma(qbuf.at[p, t, 3 if sign > 0 else 1, half], qbuf.at[p, t, 2, half],
                    *sems(p, t, 2 if sign > 0 else 3), nbr(p, False, sign))

    def send2(p, t):
        if t < 3:
            for d in ((1, 2, 3) if p == 0 else (0, 1, 2, 3)):
                (h0 if p == 0 else h1)(t, d).wait_recv()
        else:
            s = (t - 3) * 2 + p
            mine = (g == s) & (y == k)
            for d in range(4):
                n = (p * NPART + t) * 4 + d
                cp = rdma(qown.at[3], qbuf.at[p, t, 0, (4 - d) % 4], hsend.at[0], hrecv.at[n], (g, c))
                if d == 0:
                    pl.when(jnp.logical_not(mine))(cp.wait_recv)
                else:
                    cp.wait_recv()
        g2(p, t, 1).start()
        g2(p, t, -1).start()

    def relay2(p, t):
        for sign in (1, -1):
            g2(p, t, sign).wait_recv()
            g2f(p, t, sign).start()

    def ready(p, t):
        for sign in (1, -1):
            g2f(p, t, sign).wait_recv()

    order = [(0, 0), (1, 0), (0, 1), (1, 1), (0, 3), (1, 3), (0, 4), (1, 4), (1, 2), (0, 2)]
    slot_u = [u for u in order if u[1] >= 3]

    for t in range(2):
        for d in (1, 3, 2):
            h0(t, d).start()
        for d in (0, 1, 3, 2):
            h1(t, d).start()
    targets = [(hh, yy, d) for d in (0, 1, 3, 2) for hh in range(2) for yy in range(2)]
    for hh, yy, d in targets:
        if d == 0:
            mine = (2 * hh + y == g) & (y == yy)
            pl.when(jnp.logical_not(mine))(hs(hh, yy, d).start)
        else:
            hs(hh, yy, d).start()

    @pl.when(y == k)
    def _():
        qbuf[g % 2, 3 + g // 2, 0, 0] = qown[3]

    for t in range(2, 3):
        for d in (1, 3, 2):
            h0(t, d).start()
        for d in (0, 1, 3, 2):
            h1(t, d).start()
    swap = rdma(cache_ref, cbuf.at[1], csem.at[3], csem.at[4], (g + 1 - 2 * k, c))
    swap.start()
    phase("g1")
    for u in order[:4]:
        send2(*u)
    phase("g2")
    relay2(*order[0])
    for u in order[4:6]:
        send2(*u)
    relay2(*order[1])
    for u in order[6:]:
        send2(*u)
    own_copy.wait()

    nj = 4
    wj = CTX // nj
    start_pos = c * CTX

    def attend(p, t):
        if t < 3:
            keys = cbuf.at[0]
            limit = len_ref[g] - start_pos
        else:
            d = don_ref[(t - 3) * 2 + p]
            keys = cbuf.at[jnp.where(d % 2 == k, 0, 1)]
            limit = jnp.where(d // 2 == h, len_ref[d] - start_pos, 0)
        q = qbuf[p, t].reshape(UNIT, KEYW)
        top = jnp.full((UNIT, 1), FLOOR, F32)
        for j in range(nj):
            pos = lax.broadcasted_iota(jnp.int32, (1, wj), 1) + j * wj
            bias = jnp.where(pos < limit, 0.0, LOW)
            sc = jnp.dot(q, keys[:, j * wj:(j + 1) * wj], preferred_element_type=F32) * SCALE2 + bias
            scr[:, j * wj:(j + 1) * wj] = sc
            top = jnp.maximum(top, jnp.max(sc, axis=1, keepdims=True))
        top = rounded(top)
        total = jnp.zeros((UNIT, 1), F32)
        acc = jnp.zeros((UNIT, LATENT), F32)
        for j in range(nj):
            w = jnp.exp2(scr[:, j * wj:(j + 1) * wj] - top)
            total = total + jnp.sum(w, axis=1, keepdims=True)
            acc = acc + lax.dot_general(w.astype(BF), keys[:LATENT, j * wj:(j + 1) * wj],
                                        (((1,), (1,)), ((), ())), preferred_element_type=F32)
        obuf[p, t] = acc.astype(BF).reshape(4, 4, ROWS, LATENT)
        hi = rounded(total)
        lo = total - hi
        for a in range(4):
            tile = jnp.zeros((ROWS, 128), F32)
            for b in range(4):
                rows = slice((a * 4 + b) * ROWS, (a * 4 + b + 1) * ROWS)
                tile = jnp.where(lane == b, top[rows], tile)
                tile = jnp.where(lane == 4 + b, hi[rows], tile)
                tile = jnp.where(lane == 8 + b, lo[rows], tile)
            stat[p, t, a] = tile.astype(BF)

    def rsem(p, t, i):
        n = (p * NPART + t) * 8 + i
        return rsend.at[n], rrecv.at[n]

    def a1(p, t, sign):
        i = 0 if sign > 0 else 1
        half = pl.ds(0, 2) if sign > 0 else pl.ds(2, 2)
        dev = nbr(p, False, sign)
        return (rdma(obuf.at[p, t, 2, half], ra.at[p, t, i], *rsem(p, t, i), dev),
                rdma(stat.at[p, t, 2], ras.at[p, t, i], *rsem(p, t, 2 + i), dev))

    def a2(p, t, sign):
        i = 0 if sign > 0 else 1
        a = 1 if sign > 0 else 3
        dev = nbr(p, False, sign)
        return (rdma(obuf.at[p, t, a], rc.at[p, t, i], *rsem(p, t, 4 + i), dev),
                rdma(stat.at[p, t, a], rcs.at[p, t, i], *rsem(p, t, 6 + i), dev))

    def back(p, t, d):
        if t < 3:
            dev = (g, at(0, d, y) if p == 0 else at(d, 0, 1 - y))
            i = t * 7 + (d - 1 if p == 0 else 3 + d)
            return (rdma(obuf.at[p, t, 0, d], rd.at[i], dsend.at[2 * i], drecv.at[2 * i], dev),
                    rdma(stat.at[p, t, 0], rds.at[i], dsend.at[2 * i + 1], drecv.at[2 * i + 1], dev))
        s = (t - 3) * 2 + p
        dev = (s, at(0, d, k) if p == 0 else at(d, 0, k))
        i = (2 * h + y) * 4 + d
        j = 2 * (s * 4 + d)
        return (rdma(obuf.at[p, t, 0, d], rf.at[i], fsend.at[j], frecv.at[2 * i], dev),
                rdma(stat.at[p, t, 0], rfs.at[i], fsend.at[j + 1], frecv.at[2 * i + 1], dev))

    def start(pair):
        for cp in pair:
            cp.start()

    def got(pair):
        for cp in pair:
            cp.wait_recv()

    def gone(pair):
        for cp in pair:
            cp.wait_send()

    def only(pair, keep):
        return jnp.where(keep, pair[0], 4 * FLOOR), jnp.where(keep, pair[1], 0.0)

    def shifted(pair, b):
        if b == 0:
            return pair
        return pltpu.roll(pair[0], 128 - b, 1), pltpu.roll(pair[1], 128 - b, 1)

    def begin(p, t):
        start(a1(p, t, 1))
        start(a1(p, t, -1))

    def r1(p, t):
        for i, sign in ((0, 1), (1, -1)):
            got(a1(p, t, sign))
            a = 1 if i == 0 else 3
            inside = (lane < 2) if i == 0 else (lane >= 2) & (lane < 4)
            top, total, (f0, f1) = combine([stats(stat[p, t, a]), only(stats(ras[p, t, i]), inside)])
            for b in range(2):
                bb = 2 * i + b
                o = (obuf[p, t, a, bb].astype(F32) * f0[:, bb:bb + 1]
                     + ra[p, t, i, b].astype(F32) * f1[:, bb:bb + 1])
                obuf[p, t, a, bb] = o.astype(BF)
            stat[p, t, a] = packed(top, total)
            start(a2(p, t, sign))

    def r2(p, t):
        got(a2(p, t, 1))
        got(a2(p, t, -1))
        top, total, (f0, f1, f2) = combine([stats(stat[p, t, 0]), stats(rcs[p, t, 0]), stats(rcs[p, t, 1])])
        for b in (2, 1, 3, 0):
            o = (obuf[p, t, 0, b].astype(F32) * f0[:, b:b + 1] + rc[p, t, 0, b].astype(F32) * f1[:, b:b + 1]
                 + rc[p, t, 1, b].astype(F32) * f2[:, b:b + 1])
            obuf[p, t, 0, b] = o.astype(BF)
        stat[p, t, 0] = packed(top, total)
        if t < 3:
            for d in ((2, 1, 3) if p == 0 else (2, 1, 3, 0)):
                start(back(p, t, d))
        else:
            s = (t - 3) * 2 + p
            mine = (g == s) & (y == k)
            for d in (2, 1, 3):
                start(back(p, t, d))

            @pl.when(jnp.logical_not(mine))
            def _():
                start(back(p, t, 0))

            @pl.when(mine)
            def _():
                rf[(2 * h + y) * 4] = obuf[p, t, 0, 0]
                rfs[(2 * h + y) * 4] = stat[p, t, 0]

    att = [None] * 4

    def finish(t, parts, outs):
        parts = parts + [(fst[t, 0], fst[t, 1])]
        _, total, fs = combine(parts)
        o = fo[t] * fs[-1][:, 0:1]
        for f, v in zip(fs[:-1], outs):
            o = o + v().astype(F32) * f[:, 0:1]
        att[t] = (o / total[:, 0:1]).astype(BF)

    def fin_step(t):
        parts = [stats(stat[0, t, 0])]
        outs = [lambda: obuf[0, t, 0, 0]]
        for p in range(2):
            for d in ((1, 2, 3) if p == 0 else (0, 1, 2, 3)):
                got(back(p, t, d))
                i = t * 7 + (d - 1 if p == 0 else 3 + d)
                parts.append(shifted(stats(rds[i]), d))
                outs.append(functools.partial(lambda i: rd[i], i))
        finish(t, parts, outs)

    def fin_slot():
        parts, outs = [], []
        for i in range(16):
            cps = (rdma(obuf.at[0, 3, 0, 0], rf.at[i], fsend.at[0], frecv.at[2 * i], (g, c)),
                   rdma(stat.at[0, 3, 0], rfs.at[i], fsend.at[1], frecv.at[2 * i + 1], (g, c)))
            if i % 4 == 0:
                mine = (y == k) & (i // 4 == 2 * h + y)
                pl.when(jnp.logical_not(mine))(functools.partial(got, cps))
            else:
                got(cps)
            parts.append(shifted(stats(rfs[i]), i % 4))
            outs.append(functools.partial(lambda i: rf[i], i))
        finish(3, parts, outs)

    n_units = len(order)
    relayed = order[:2]
    lag1, lag2 = 2, 4
    for i in range(n_units + lag2):
        phase("r%d" % i)
        if lag2 <= i:
            r2(*order[i - lag2])
        if lag1 <= i < n_units + lag1:
            r1(*order[i - lag1])
        if i < n_units:
            for u in order[:i + 3]:
                if u not in relayed:
                    relay2(*u)
                    relayed.append(u)
            phase("w%d" % i)
            ready(*order[i])
            if order[i] == slot_u[0]:
                swap.wait()
            phase("attend%d" % i)
            attend(*order[i])
            begin(*order[i])
        if i == n_units:
            phase("fin0")
            fin_step(0)
            fin_step(1)
    phase("fin")
    fin_slot()
    fin_step(2)

    phase("tail")
    attended = jnp.concatenate(att, axis=0)
    vu_copy.wait()
    op_copy.wait()
    row_head = lax.broadcasted_iota(jnp.int32, (64, 128), 0) % 4
    pieces = []
    for head in range(4):
        hv = jnp.dot(attended, vuv[head], preferred_element_type=F32)
        pieces.append(jnp.where(row_head == head, hv, 0.0).astype(BF))
    spread = jnp.concatenate(pieces, axis=1)
    pick = (lax.broadcasted_iota(jnp.int32, (ROWS, 64), 1) // 4
            == lax.broadcasted_iota(jnp.int32, (ROWS, 64), 0))
    joined = jnp.dot(jnp.where(pick, 1.0, 0.0).astype(BF), spread, preferred_element_type=F32).astype(BF)

    def outc(dest, rel):
        return rdma(sbuf.at[dest], rbuf.at[rel], xsend.at[dest], xrecv.at[rel], (g, dest))

    width = 8 * OUTW
    for blk in range(4):
        term = jnp.dot(joined, opv[:, blk * width:(blk + 1) * width], preferred_element_type=F32)
        for i in range(8):
            sbuf[blk * 8 + i, :, :OUTW] = term[:, i * OUTW:(i + 1) * OUTW].astype(BF)

    def send_out(i, carry):
        outc((c + i) % NPEER, (NPEER - i) % NPEER).start()
        return carry

    lax.fori_loop(1, NPEER, send_out, 0)
    phase("outx")

    for hh, yy, d in targets:
        if d == 0:
            mine = (2 * hh + y == g) & (y == yy)
            pl.when(jnp.logical_not(mine))(hs(hh, yy, d).wait_send)
        else:
            hs(hh, yy, d).wait_send()
    for p, t in order:
        if t < 3:
            for d in ((1, 2, 3) if p == 0 else (0, 1, 2, 3)):
                (h0 if p == 0 else h1)(t, d).wait_send()
                gone(back(p, t, d))
        else:
            for d in (1, 2, 3):
                gone(back(p, t, d))
            mine = (g == (t - 3) * 2 + p) & (y == k)
            pl.when(jnp.logical_not(mine))(functools.partial(gone, back(p, t, 0)))
        for sign in (1, -1):
            g2(p, t, sign).wait_send()
            g2f(p, t, sign).wait_send()
            gone(a1(p, t, sign))
            gone(a2(p, t, sign))

    res = sbuf[c][:, :OUTW].astype(F32)
    for rel in range(1, NPEER):
        pltpu.make_async_remote_copy(src_ref=sbuf.at[0], dst_ref=rbuf.at[rel], send_sem=xsend.at[0],
                                     recv_sem=xrecv.at[rel], device_id=(g, c), device_id_type=MESH).wait_recv()
        res = res + rbuf[rel][:, :OUTW].astype(F32)
    for t in range(4):
        out_ref[t, 0] = res[4 * t:4 * t + 4].astype(BF)

    def sent_out(i, carry):
        outc((c + i) % NPEER, (NPEER - i) % NPEER).wait_send()
        return carry

    lax.fori_loop(1, NPEER, sent_out, 0)
    phase(None)


def body(cache, queries, new_latent, lengths, donor, value_up, out_proj):
    keys = jnp.swapaxes(cache[0], 0, 1)
    VM, SM, ANY = pltpu.VMEM, pltpu.SMEM, pl.ANY
    U = (2, NPART)
    dma = pltpu.SemaphoreType.DMA
    return pl.pallas_call(
        kernel,
        out_shape=jax.ShapeDtypeStruct((4, 1, 4, OUTW), BF),
        in_specs=[pl.BlockSpec(memory_space=m) for m in (SM, SM, VM, VM, ANY, ANY, ANY)],
        out_specs=pl.BlockSpec(memory_space=VM),
        scratch_shapes=[
            VM((2, KEYW, CTX), BF),
            VM((4, ROWS, KEYW), BF),
            VM(U + (4, 4, ROWS, KEYW), BF),
            VM(U + (4, 4, ROWS, LATENT), BF),
            VM(U + (4, ROWS, 128), BF),
            VM(U + (2, 2, ROWS, LATENT), BF), VM(U + (2, ROWS, 128), BF),
            VM(U + (2, 4, ROWS, LATENT), BF), VM(U + (2, ROWS, 128), BF),
            VM((21, ROWS, LATENT), BF), VM((21, ROWS, 128), BF),
            VM((16, ROWS, LATENT), BF), VM((16, ROWS, 128), BF),
            VM((NPEER, ROWS, 256), BF), VM((NPEER, ROWS, 256), BF),
            VM((512, 7168), BF), VM((4, LATENT, 128), BF),
            VM((UNIT, CTX), F32),
            VM((4, ROWS, LATENT), F32), VM((4, 2, ROWS, 128), F32),
            dma((5,)), dma((56,)), dma((40,)), dma((40,)), dma((40,)), dma((80,)), dma((80,)),
            dma((NPEER,)), dma((NPEER,)), dma((42,)), dma((42,)), dma((32,)), dma((32,)),
        ],
        compiler_params=pltpu.CompilerParams(collective_id=0, has_side_effects=True,
                                             vmem_limit_bytes=56 * 1024 * 1024),
        name="mla_step",
    )(lengths, donor, queries, new_latent, keys, value_up, out_proj)


def solution(mesh):
    return jax.shard_map(
        body,
        mesh=mesh,
        in_specs=(
            P("grp", "ctx", None),
            P(None, "grp", None, "ctx", None),
            P(None, "grp", None, None),
            P(),
            P(),
            P("ctx", None, None),
            P("ctx", None),
        ),
        out_specs=P(None, "grp", None, "ctx"),
        check_vma=False,
    )
```

```python
import functools

import jax
import jax.numpy as jnp
from jax import lax
from jax.experimental import pallas as pl
from jax.experimental.pallas import tpu as pltpu
from jax.sharding import PartitionSpec as P

MESH = pl.DeviceIdType.MESH
LATENT = 512
KEYW = 576
CTX = 2048
ROWS = 16
UNIT = 256
NPART = 5
OUTW = 224
NPEER = 32
SCALE2 = (192.0 ** -0.5) * 1.4426950408889634
LOW = -1e30
FLOOR = -1e29
BF = jnp.bfloat16
F32 = jnp.float32


def rounded(v):
    return v.astype(BF).astype(F32)


def lanes_of(shape):
    return lax.broadcasted_iota(jnp.int32, shape, 1)


def stats(tile):
    t = tile.astype(F32)
    return t, pltpu.roll(t, 124, 1) + pltpu.roll(t, 120, 1)


def combine(parts):
    top = parts[0][0]
    for t, _ in parts[1:]:
        top = jnp.maximum(top, t)
    factors = [jnp.exp2(t - top) for t, _ in parts]
    total = factors[0] * parts[0][1]
    for f, (_, v) in zip(factors[1:], parts[1:]):
        total = total + f * v
    return top, total, factors


def packed(top, total):
    lane = lanes_of(top.shape)
    hi = rounded(total)
    lo = total - hi
    return jnp.where(lane < 4, top, jnp.where(lane < 8, pltpu.roll(hi, 4, 1), pltpu.roll(lo, 8, 1))).astype(BF)


def kernel(len_ref, don_ref, q_ref, nl_ref, cache_ref, vu_ref, op_ref, out_ref,
           cbuf, qown, qbuf, obuf, stat, ra, ras, rc, rcs, rd, rds, rf, rfs,
           sbuf, rbuf, opv, vuv, fo, fst,
           csem, hsend, hrecv, gsend, grecv, rsend, rrecv, xsend, xrecv, dsend, drecv, fsend, frecv):
    g = lax.axis_index("grp")
    c = lax.axis_index("ctx")
    h = g // 2
    k = g % 2
    z = c // 8
    x = (c // 2) % 4
    y = c % 2
    other = c + 1 - 2 * y

    def at(dz, dx, yy):
        return ((z + dz + 4) % 4) * 8 + ((x + dx + 4) % 4) * 2 + yy

    def line(p, t, d):
        return (0, d) if (p + t) % 2 == 0 else (d, 0)

    def nbr(p, t, d):
        dx, dz = line(p, t, d)
        return (g, at(dz, dx, y))

    def rdma(src, dst, ss, rs, dev):
        return pltpu.make_async_remote_copy(src_ref=src, dst_ref=dst, send_sem=ss, recv_sem=rs,
                                            device_id=dev, device_id_type=MESH)

    scope = [None]

    def phase(name):
        if scope[0] is not None:
            scope[0].__exit__(None, None, None)
            scope[0] = None
        if name:
            scope[0] = jax.named_scope(name)
            scope[0].__enter__()

    phase("enter")
    barrier = pltpu.get_barrier_semaphore()

    def greet(i, carry):
        pl.semaphore_signal(barrier, inc=1, device_id=(g, (c + i) % NPEER), device_id_type=MESH)
        return carry

    lax.fori_loop(1, NPEER, greet, 0)
    places = [(0, 0)] + [(d, 0) for d in range(1, 4)] + [(0, d) for d in range(1, 4)]
    for dg in range(1, 4):
        for dz, dx in places:
            for yy in range(2):
                pl.semaphore_signal(barrier, inc=1, device_id=((g + dg) % 4, at(dz, dx, yy)), device_id_type=MESH)

    own_copy = pltpu.make_async_copy(cache_ref, cbuf.at[0], csem.at[0])
    own_copy.start()
    vu_copy = pltpu.make_async_copy(vu_ref, vuv, csem.at[2])
    vu_copy.start()
    op_copy = pltpu.make_async_copy(op_ref, opv, csem.at[1])
    op_copy.start()
    for t in range(4):
        for s in range(4):
            qown[t, 4 * s:4 * s + 4] = q_ref[t, 0, s]
    for t in range(3):
        qbuf[0, t, 0, 0] = qown[t]

    lane = lanes_of((ROWS, 128))
    lane_k = lanes_of((ROWS, 4))
    row_s = lax.broadcasted_iota(jnp.int32, (ROWS, 4), 0) // 4
    for t in range(4):
        q = qown[t]
        logits = []
        for u in range(t + 1):
            lg = lax.dot_general(q, nl_ref[u, 0], (((1,), (1,)), ((), ())), preferred_element_type=F32)
            logits.append(jnp.where(lane_k == row_s, lg * SCALE2, LOW))
        top = jnp.max(logits[0], axis=1, keepdims=True)
        for lg in logits[1:]:
            top = jnp.maximum(top, jnp.max(lg, axis=1, keepdims=True))
        total = jnp.zeros((ROWS, 1), F32)
        acc = jnp.zeros((ROWS, LATENT), F32)
        for u in range(t + 1):
            w = jnp.where(lane_k == row_s, jnp.exp2(logits[u] - top), 0.0)
            total = total + jnp.sum(w, axis=1, keepdims=True)
            val = nl_ref[u, 0][:, :LATENT]
            whi = w.astype(BF)
            wlo = (w - whi.astype(F32)).astype(BF)
            acc = acc + (jnp.dot(whi, val, preferred_element_type=F32)
                         + jnp.dot(wlo, val, preferred_element_type=F32))
        fo[t] = acc
        fst[t, 0] = jnp.broadcast_to(top, (ROWS, 128))
        fst[t, 1] = jnp.broadcast_to(total, (ROWS, 128))

    pl.semaphore_wait(barrier, NPEER - 1 + 42)
    phase("prep")

    def hsems(p, t, d):
        n = (p * NPART + t) * 4 + d
        return hsend.at[n], hrecv.at[n]

    def along(p, t, d):
        dz, dx = line(p, t, d)
        return rdma(qbuf.at[p, t, 0, 0], qbuf.at[p, t, 0, (4 - d) % 4], *hsems(p, t, d), (g, at(dz, dx, y)))

    def across(t):
        return rdma(qown.at[t], qbuf.at[1, t, 0, 0], *hsems(1, t, 0), (g, other))

    def handed(hh, yy):
        n = ((g % 2) * NPART + 3 + g // 2) * 4
        return rdma(qown.at[3], qbuf.at[g % 2, 3 + g // 2, 0, 0],
                    hsend.at[40 + 2 * hh + yy], hrecv.at[n], (2 * hh + y, at(0, 0, yy)))

    def handed_in(p, t):
        n = (p * NPART + t) * 4
        return rdma(qown.at[3], qbuf.at[p, t, 0, 0], hsend.at[0], hrecv.at[n], (g, c))

    def sems(p, t, i):
        n = (p * NPART + t) * 4 + i
        return gsend.at[n], grecv.at[n]

    def g2(p, t, sign):
        return rdma(qbuf.at[p, t, 0], qbuf.at[p, t, 3 if sign > 0 else 1],
                    *sems(p, t, 0 if sign > 0 else 1), nbr(p, t, sign))

    def g2f(p, t, sign):
        half = pl.ds(0, 2) if sign > 0 else pl.ds(2, 2)
        return rdma(qbuf.at[p, t, 3 if sign > 0 else 1, half], qbuf.at[p, t, 2, half],
                    *sems(p, t, 2 if sign > 0 else 3), nbr(p, t, sign))

    def send1(p, t):
        for d in (1, 3, 2):
            along(p, t, d).start()

    def send2(p, t):
        for d in range(1, 4):
            along(p, t, d).wait_recv()
        g2(p, t, 1).start()
        g2(p, t, -1).start()

    def spread(p, t):
        if t < 3:
            across(t).wait_recv()
        else:
            mine = (g == (t - 3) * 2 + p) & (y == k)
            pl.when(jnp.logical_not(mine))(handed_in(p, t).wait_recv)
        send1(p, t)

    def relay2(p, t):
        for sign in (1, -1):
            g2(p, t, sign).wait_recv()
            g2f(p, t, sign).start()

    def ready(p, t):
        for sign in (1, -1):
            g2f(p, t, sign).wait_recv()

    early = [(0, 0), (0, 1)]
    middle = [(1, 0), (1, 1)]
    late = [(1, 2), (0, 2)]
    slot_u = [(0, 3), (1, 3), (0, 4), (1, 4)]
    order = early + middle + slot_u + late

    def handed_do(what):
        for hh in range(2):
            for yy in range(2):
                mine = (2 * hh + y == g) & (y == yy)
                cp = handed(hh, yy)
                pl.when(jnp.logical_not(mine))(cp.start if what else cp.wait_send)

    across(0).start()
    across(1).start()
    send1(0, 0)
    send1(0, 1)
    across(2).start()
    handed_do(True)
    send1(0, 2)

    @pl.when(y == k)
    def _():
        qbuf[g % 2, 3 + g // 2, 0, 0] = qown[3]

    swap = rdma(cache_ref, cbuf.at[1], csem.at[3], csem.at[4], (g + 1 - 2 * k, c))

    nj = 2
    wj = CTX // nj
    start_pos = c * CTX

    def attend(groups):
        n = len(groups)
        p, t, _ = groups[0]
        if t < 3:
            keys = cbuf.at[0]
            limit = len_ref[g] - start_pos
        else:
            d = don_ref[(t - 3) * 2 + p]
            keys = cbuf.at[jnp.where(d % 2 == k, 0, 1)]
            limit = jnp.where(d // 2 == h, len_ref[d] - start_pos, 0)
        q = jnp.concatenate([qbuf[p, t, a].reshape(64, KEYW) for p, t, a in groups], axis=0)

        def score(j):
            pos = lax.broadcasted_iota(jnp.int32, (1, wj), 1) + j * wj
            bias = jnp.where(pos < limit, 0.0, LOW)
            return jnp.dot(q, keys[:, j * wj:(j + 1) * wj], preferred_element_type=F32) * SCALE2 + bias

        top = total = acc = None
        later = score(0)
        for j in range(nj):
            sc = later
            if j + 1 < nj:
                later = score(j + 1)
            peak = rounded(jnp.maximum(jnp.max(sc, axis=1, keepdims=True), FLOOR if top is None else top))
            w = jnp.exp2(sc - peak)
            part = jnp.sum(w, axis=1, keepdims=True)
            val = lax.dot_general(w.astype(BF), keys[:LATENT, j * wj:(j + 1) * wj],
                                  (((1,), (1,)), ((), ())), preferred_element_type=F32)
            if top is None:
                total, acc = part, val
            else:
                scale = jnp.exp2(top - peak)
                total = total * scale + part
                acc = acc * scale + val
            top = peak
        hi = rounded(total)
        lo = total - hi
        for i, (p, t, a) in enumerate(groups):
            obuf[p, t, a] = acc[64 * i:64 * i + 64].astype(BF).reshape(4, ROWS, LATENT)
            tile = jnp.zeros((ROWS, 128), F32)
            for b in range(4):
                part = slice((i * 4 + b) * ROWS, (i * 4 + b + 1) * ROWS)
                tile = jnp.where(lane == b, top[part], tile)
                tile = jnp.where(lane == 4 + b, hi[part], tile)
                tile = jnp.where(lane == 8 + b, lo[part], tile)
            stat[p, t, a] = tile.astype(BF)

    def rsem(p, t, i):
        n = (p * NPART + t) * 8 + i
        return rsend.at[n], rrecv.at[n]

    def a1(p, t, sign):
        i = 0 if sign > 0 else 1
        half = pl.ds(0, 2) if sign > 0 else pl.ds(2, 2)
        dev = nbr(p, t, sign)
        return (rdma(obuf.at[p, t, 2, half], ra.at[p, t, i], *rsem(p, t, i), dev),
                rdma(stat.at[p, t, 2], ras.at[p, t, i], *rsem(p, t, 2 + i), dev))

    def a2(p, t, sign):
        i = 0 if sign > 0 else 1
        a = 1 if sign > 0 else 3
        dev = nbr(p, t, sign)
        return (rdma(obuf.at[p, t, a], rc.at[p, t, i], *rsem(p, t, 4 + i), dev),
                rdma(stat.at[p, t, a], rcs.at[p, t, i], *rsem(p, t, 6 + i), dev))

    def back(p, t, d):
        dz, dx = line(p, t, d)
        if t < 3:
            dev = (g, at(dz, dx, y if p == 0 else 1 - y))
            i = t * 7 + (d - 1 if p == 0 else 3 + d)
            return (rdma(obuf.at[p, t, 0, d], rd.at[i], dsend.at[2 * i], drecv.at[2 * i], dev),
                    rdma(stat.at[p, t, 0], rds.at[i], dsend.at[2 * i + 1], drecv.at[2 * i + 1], dev))
        s = (t - 3) * 2 + p
        dev = (s, at(dz, dx, k))
        i = (2 * h + y) * 4 + d
        j = 2 * (s * 4 + d)
        return (rdma(obuf.at[p, t, 0, d], rf.at[i], fsend.at[j], frecv.at[2 * i], dev),
                rdma(stat.at[p, t, 0], rfs.at[i], fsend.at[j + 1], frecv.at[2 * i + 1], dev))

    def start(pair):
        for cp in pair:
            cp.start()

    def got(pair):
        for cp in pair:
            cp.wait_recv()

    def gone(pair):
        for cp in pair:
            cp.wait_send()

    def only(pair, keep):
        return jnp.where(keep, pair[0], 4 * FLOOR), jnp.where(keep, pair[1], 0.0)

    def shifted(pair, b):
        if b == 0:
            return pair
        return pltpu.roll(pair[0], 128 - b, 1), pltpu.roll(pair[1], 128 - b, 1)

    def begin(p, t):
        start(a1(p, t, 1))
        start(a1(p, t, -1))

    def r1(units):
        for p, t in units:
            got(a1(p, t, 1))
            got(a1(p, t, -1))
        for p, t in units:
            for i in range(2):
                a = 1 if i == 0 else 3
                inside = (lane < 2) if i == 0 else (lane >= 2) & (lane < 4)
                top, total, (f0, f1) = combine([stats(stat[p, t, a]), only(stats(ras[p, t, i]), inside)])
                for b in range(2):
                    bb = 2 * i + b
                    o = (obuf[p, t, a, bb].astype(F32) * f0[:, bb:bb + 1]
                         + ra[p, t, i, b].astype(F32) * f1[:, bb:bb + 1])
                    obuf[p, t, a, bb] = o.astype(BF)
                stat[p, t, a] = packed(top, total)
        for p, t in units:
            start(a2(p, t, 1))
            start(a2(p, t, -1))

    def r2(units):
        for p, t in units:
            got(a2(p, t, 1))
            got(a2(p, t, -1))
        for p, t in units:
            top, total, (f0, f1, f2) = combine([stats(stat[p, t, 0]), stats(rcs[p, t, 0]), stats(rcs[p, t, 1])])
            for b in range(4):
                o = (obuf[p, t, 0, b].astype(F32) * f0[:, b:b + 1] + rc[p, t, 0, b].astype(F32) * f1[:, b:b + 1]
                     + rc[p, t, 1, b].astype(F32) * f2[:, b:b + 1])
                obuf[p, t, 0, b] = o.astype(BF)
            stat[p, t, 0] = packed(top, total)
        for p, t in units:
            for d in (2, 1, 3):
                start(back(p, t, d))
            if t < 3:
                if p == 1:
                    start(back(p, t, 0))
            else:
                mine = (g == (t - 3) * 2 + p) & (y == k)

                @pl.when(jnp.logical_not(mine))
                def _():
                    start(back(p, t, 0))

                @pl.when(mine)
                def _():
                    rf[(2 * h + y) * 4] = obuf[p, t, 0, 0]
                    rfs[(2 * h + y) * 4] = stat[p, t, 0]

    att = [None] * 4

    def fold_in(t, parts, outs, last):
        parts = parts + [(fst[t, 0], fst[t, 1])]
        top, total, fs = combine(parts)
        o = fo[t] * fs[-1][:, 0:1]
        for f, v in zip(fs[:-1], outs):
            o = o + v.astype(F32) * f[:, 0:1]
        if last:
            att[t] = (o / total[:, 0:1]).astype(BF)
        else:
            fo[t] = o
            fst[t, 0] = top
            fst[t, 1] = total

    def fin_half(p, t):
        ds = (1, 2, 3) if p == 0 else (0, 1, 2, 3)
        for d in ds:
            got(back(p, t, d))
        where = [t * 7 + (d - 1 if p == 0 else 3 + d) for d in ds]
        parts = [shifted(stats(rds[i]), d) for i, d in zip(where, ds)]
        outs = [rd[i] for i in where]
        if p == 0:
            parts.append(stats(stat[0, t, 0]))
            outs.append(obuf[0, t, 0, 0])
        fold_in(t, parts, outs, p == 1)

    def fin_slot():
        for i in range(16):
            cps = (rdma(obuf.at[0, 3, 0, 0], rf.at[i], fsend.at[0], frecv.at[2 * i], (g, c)),
                   rdma(stat.at[0, 3, 0], rfs.at[i], fsend.at[1], frecv.at[2 * i + 1], (g, c)))
            if i % 4 == 0:
                mine = (y == k) & (i // 4 == 2 * h + y)
                pl.when(jnp.logical_not(mine))(functools.partial(got, cps))
            else:
                got(cps)
        fold_in(3, [shifted(stats(rfs[i]), i % 4) for i in range(16)], [rf[i] for i in range(16)], True)

    def each(f, units):
        for u in units:
            f(*u)

    def of(units, *dists):
        return [(p, t, a) for a in dists for p, t in units]

    phase("g1")
    each(spread, middle)
    each(send2, early)
    spread(*late[0])
    each(spread, slot_u)
    own_copy.wait()
    phase("B1")
    attend(of(early, 0))
    phase("g2")
    each(send2, middle)
    each(relay2, early)
    each(send2, late)
    swap.start()
    phase("B2")
    attend(of(early, 1, 3))
    phase("g3")
    each(send2, slot_u[:2])
    each(relay2, middle)
    each(send2, slot_u[2:])
    each(ready, early)
    phase("B3")
    attend(of(early, 2) + of(middle, 0))
    each(begin, early)
    phase("g4")
    each(relay2, late)
    phase("B4")
    attend(of(middle, 1, 3))
    phase("g5")
    each(relay2, slot_u[:2])
    each(ready, middle)
    each(ready, late)
    phase("B5")
    attend(of(middle, 2) + of(late, 2))
    each(begin, middle)
    each(begin, late)
    phase("g6")
    each(relay2, slot_u[2:])
    r1(early)
    swap.wait()

    def slot(i):
        phase("ws%d" % i)
        ready(*slot_u[i])
        phase("S%d" % i)
        attend(of(slot_u[i:i + 1], 0, 1, 2, 3))
        begin(*slot_u[i])
        phase("rs%d" % i)

    slot(0)
    slot(1)
    r1(middle)
    r2(early)
    slot(2)
    r1(slot_u[0:1])
    slot(3)
    r1(slot_u[1:2])
    r2(middle)
    phase("M3")
    attend(of(late, 1, 3) + of(late[:1], 0))
    phase("rm3")
    r1(late)
    r1(slot_u[2:3])
    r2(slot_u[0:1])
    fin_half(0, 0)
    fin_half(0, 1)
    phase("E")
    attend(of(late[1:], 0))
    phase("re")
    r1(slot_u[3:])
    r2(slot_u[1:2])
    fin_half(1, 0)
    fin_half(1, 1)
    phase("rlate")
    r2(late)
    phase("rs12")
    r2(slot_u[2:3])
    phase("rs13")
    r2(slot_u[3:])
    phase("f2")
    fin_half(0, 2)
    fin_half(1, 2)
    phase("fs")
    fin_slot()

    phase("tail")
    attended = jnp.concatenate(att, axis=0)
    vu_copy.wait()
    op_copy.wait()
    row_head = lax.broadcasted_iota(jnp.int32, (64, 128), 0) % 4
    pieces = []
    for head in range(4):
        hv = jnp.dot(attended, vuv[head], preferred_element_type=F32)
        pieces.append(jnp.where(row_head == head, hv, 0.0).astype(BF))
    spread = jnp.concatenate(pieces, axis=1)
    pick = (lax.broadcasted_iota(jnp.int32, (ROWS, 64), 1) // 4
            == lax.broadcasted_iota(jnp.int32, (ROWS, 64), 0))
    joined = jnp.dot(jnp.where(pick, 1.0, 0.0).astype(BF), spread, preferred_element_type=F32).astype(BF)

    def outc(dest, rel):
        return rdma(sbuf.at[dest], rbuf.at[rel], xsend.at[dest], xrecv.at[rel], (g, dest))

    width = 8 * OUTW
    for blk in range(4):
        term = jnp.dot(joined, opv[:, blk * width:(blk + 1) * width], preferred_element_type=F32)
        for i in range(8):
            dest = blk * 8 + i
            sbuf[dest, :, :OUTW] = term[:, i * OUTW:(i + 1) * OUTW].astype(BF)
        for i in range(8):
            dest = blk * 8 + i
            pl.when(dest != c)(outc(dest, (c - dest + NPEER) % NPEER).start)
    phase("outx")

    handed_do(False)
    for p, t in order:
        for d in (1, 2, 3):
            along(p, t, d).wait_send()
            gone(back(p, t, d))
        if t >= 3:
            mine = (g == (t - 3) * 2 + p) & (y == k)
            pl.when(jnp.logical_not(mine))(functools.partial(gone, back(p, t, 0)))
        elif p == 1:
            across(t).wait_send()
            gone(back(p, t, 0))
        for sign in (1, -1):
            g2(p, t, sign).wait_send()
            g2f(p, t, sign).wait_send()
            gone(a1(p, t, sign))
            gone(a2(p, t, sign))

    res = sbuf[c][:, :OUTW].astype(F32)
    for rel in range(1, NPEER):
        pltpu.make_async_remote_copy(src_ref=sbuf.at[0], dst_ref=rbuf.at[rel], send_sem=xsend.at[0],
                                     recv_sem=xrecv.at[rel], device_id=(g, c), device_id_type=MESH).wait_recv()
        res = res + rbuf[rel][:, :OUTW].astype(F32)
    for t in range(4):
        out_ref[t, 0] = res[4 * t:4 * t + 4].astype(BF)

    def sent_out(i, carry):
        outc((c + i) % NPEER, (NPEER - i) % NPEER).wait_send()
        return carry

    lax.fori_loop(1, NPEER, sent_out, 0)
    phase(None)


def body(cache, queries, new_latent, lengths, donor, value_up, out_proj):
    keys = jnp.swapaxes(cache[0], 0, 1)
    VM, SM, ANY = pltpu.VMEM, pltpu.SMEM, pl.ANY
    U = (2, NPART)
    dma = pltpu.SemaphoreType.DMA
    return pl.pallas_call(
        kernel,
        out_shape=jax.ShapeDtypeStruct((4, 1, 4, OUTW), BF),
        in_specs=[pl.BlockSpec(memory_space=m) for m in (SM, SM, VM, VM, ANY, ANY, ANY)],
        out_specs=pl.BlockSpec(memory_space=VM),
        scratch_shapes=[
            VM((2, KEYW, CTX), BF),
            VM((4, ROWS, KEYW), BF),
            VM(U + (4, 4, ROWS, KEYW), BF),
            VM(U + (4, 4, ROWS, LATENT), BF),
            VM(U + (4, ROWS, 128), BF),
            VM(U + (2, 2, ROWS, LATENT), BF), VM(U + (2, ROWS, 128), BF),
            VM(U + (2, 4, ROWS, LATENT), BF), VM(U + (2, ROWS, 128), BF),
            VM((21, ROWS, LATENT), BF), VM((21, ROWS, 128), BF),
            VM((16, ROWS, LATENT), BF), VM((16, ROWS, 128), BF),
            VM((NPEER, ROWS, 256), BF), VM((NPEER, ROWS, 256), BF),
            VM((512, 7168), BF), VM((4, LATENT, 128), BF),
            VM((4, ROWS, LATENT), F32), VM((4, 2, ROWS, 128), F32),
            dma((5,)), dma((44,)), dma((40,)), dma((40,)), dma((40,)), dma((80,)), dma((80,)),
            dma((NPEER,)), dma((NPEER,)), dma((42,)), dma((42,)), dma((32,)), dma((32,)),
        ],
        compiler_params=pltpu.CompilerParams(collective_id=0, has_side_effects=True,
                                             vmem_limit_bytes=56 * 1024 * 1024),
        name="mla_step",
    )(lengths, donor, queries, new_latent, keys, value_up, out_proj)


def solution(mesh):
    return jax.shard_map(
        body,
        mesh=mesh,
        in_specs=(
            P("grp", "ctx", None),
            P(None, "grp", None, "ctx", None),
            P(None, "grp", None, None),
            P(),
            P(),
            P("ctx", None, None),
            P("ctx", None),
        ),
        out_specs=P(None, "grp", None, "ctx"),
        check_vma=False,
    )
```

```python
import functools

import jax
import jax.numpy as jnp
from jax import lax
from jax.experimental import pallas as pl
from jax.experimental.pallas import tpu as pltpu
from jax.sharding import PartitionSpec as P

MESH = pl.DeviceIdType.MESH
LATENT = 512
KEYW = 576
CTX = 2048
ROWS = 16
UNIT = 256
NPART = 5
OUTW = 224
NPEER = 32
SCALE2 = (192.0 ** -0.5) * 1.4426950408889634
LOW = -1e30
FLOOR = -1e29
BF = jnp.bfloat16
F32 = jnp.float32
XLINE = ((0, 0), (1, 0), (0, 2), (1, 3), (0, 4))


def rounded(v):
    return v.astype(BF).astype(F32)


def lanes_of(shape):
    return lax.broadcasted_iota(jnp.int32, shape, 1)


def stats(tile):
    t = tile.astype(F32)
    return t, pltpu.roll(t, 124, 1) + pltpu.roll(t, 120, 1)


TILE = (0, 4, 9, 13)
STAT = 8


def chunk(tiles):
    return jnp.concatenate(tiles, axis=1).astype(F32)


def combine(parts):
    top = parts[0][0]
    for t, _ in parts[1:]:
        top = jnp.maximum(top, t)
    factors = [jnp.exp2(t - top) for t, _ in parts]
    total = factors[0] * parts[0][1]
    for f, (_, v) in zip(factors[1:], parts[1:]):
        total = total + f * v
    return top, total, factors


def packed(top, total):
    lane = lanes_of(top.shape)
    hi = rounded(total)
    lo = total - hi
    return jnp.where(lane < 4, top, jnp.where(lane < 8, pltpu.roll(hi, 4, 1), pltpu.roll(lo, 8, 1))).astype(BF)


def kernel(len_ref, don_ref, q_ref, nl_ref, cache_ref, vu_ref, op_ref, out_ref,
           cbuf, qown, qbuf, obuf, ra, rc, bb, by, rd, rf, sbuf, rbuf, opv, vuv, fo, fst,
           csem, hsend, hrecv, gsend, grecv, rsend, rrecv, xsend, xrecv, dsend, drecv, fsend, frecv):
    g = lax.axis_index("grp")
    c = lax.axis_index("ctx")
    h = g // 2
    k = g % 2
    z = c // 8
    x = (c // 2) % 4
    y = c % 2
    other = c + 1 - 2 * y

    def at(dz, dx, yy):
        return ((z + dz + 4) % 4) * 8 + ((x + dx + 4) % 4) * 2 + yy

    def line(p, t, d):
        return (0, d) if (p, t) in XLINE else (d, 0)

    def nbr(p, t, d):
        dx, dz = line(p, t, d)
        return (g, at(dz, dx, y))

    def rdma(src, dst, ss, rs, dev):
        return pltpu.make_async_remote_copy(src_ref=src, dst_ref=dst, send_sem=ss, recv_sem=rs,
                                            device_id=dev, device_id_type=MESH)

    scope = [None]

    def phase(name):
        if scope[0] is not None:
            scope[0].__exit__(None, None, None)
            scope[0] = None
        if name:
            scope[0] = jax.named_scope(name)
            scope[0].__enter__()

    phase("enter")
    barrier = pltpu.get_barrier_semaphore()

    def greet(i, carry):
        pl.semaphore_signal(barrier, inc=1, device_id=(g, (c + i) % NPEER), device_id_type=MESH)
        return carry

    lax.fori_loop(1, NPEER, greet, 0)
    places = [(0, 0)] + [(d, 0) for d in range(1, 4)] + [(0, d) for d in range(1, 4)]
    for dg in range(1, 4):
        for dz, dx in places:
            for yy in range(2):
                pl.semaphore_signal(barrier, inc=1, device_id=((g + dg) % 4, at(dz, dx, yy)), device_id_type=MESH)

    own_copy = pltpu.make_async_copy(cache_ref, cbuf.at[0], csem.at[0])
    own_copy.start()
    vu_copy = pltpu.make_async_copy(vu_ref, vuv, csem.at[2])
    vu_copy.start()
    op_copy = pltpu.make_async_copy(op_ref, opv, csem.at[1])
    op_copy.start()
    for t in range(4):
        for s in range(4):
            qown[t, 4 * s:4 * s + 4] = q_ref[t, 0, s]
    for t in range(3):
        qbuf[0, t, 0, 0] = qown[t]

    lane = lanes_of((ROWS, 128))
    lane_k = lanes_of((ROWS, 4))
    row_s = lax.broadcasted_iota(jnp.int32, (ROWS, 4), 0) // 4
    for t in range(4):
        q = qown[t]
        logits = []
        for u in range(t + 1):
            lg = lax.dot_general(q, nl_ref[u, 0], (((1,), (1,)), ((), ())), preferred_element_type=F32)
            logits.append(jnp.where(lane_k == row_s, lg * SCALE2, LOW))
        top = jnp.max(logits[0], axis=1, keepdims=True)
        for lg in logits[1:]:
            top = jnp.maximum(top, jnp.max(lg, axis=1, keepdims=True))
        total = jnp.zeros((ROWS, 1), F32)
        acc = jnp.zeros((ROWS, LATENT), F32)
        for u in range(t + 1):
            w = jnp.where(lane_k == row_s, jnp.exp2(logits[u] - top), 0.0)
            total = total + jnp.sum(w, axis=1, keepdims=True)
            val = nl_ref[u, 0][:, :LATENT]
            whi = w.astype(BF)
            wlo = (w - whi.astype(F32)).astype(BF)
            acc = acc + (jnp.dot(whi, val, preferred_element_type=F32)
                         + jnp.dot(wlo, val, preferred_element_type=F32))
        fo[t] = acc
        fst[t, 0] = jnp.broadcast_to(top, (ROWS, 128))
        fst[t, 1] = jnp.broadcast_to(total, (ROWS, 128))

    pl.semaphore_wait(barrier, NPEER - 1 + 42)
    phase("prep")

    def hsems(p, t, d):
        n = (p * NPART + t) * 4 + d
        return hsend.at[n], hrecv.at[n]

    def along(p, t, d):
        dz, dx = line(p, t, d)
        return rdma(qbuf.at[p, t, 0, 0], qbuf.at[p, t, 0, (4 - d) % 4], *hsems(p, t, d), (g, at(dz, dx, y)))

    def across(t):
        return rdma(qown.at[t], qbuf.at[1, t, 0, 0], *hsems(1, t, 0), (g, other))

    def handed(hh, yy):
        n = ((g % 2) * NPART + 3 + g // 2) * 4
        return rdma(qown.at[3], qbuf.at[g % 2, 3 + g // 2, 0, 0],
                    hsend.at[40 + 2 * hh + yy], hrecv.at[n], (2 * hh + y, at(0, 0, yy)))

    def handed_in(p, t):
        n = (p * NPART + t) * 4
        return rdma(qown.at[3], qbuf.at[p, t, 0, 0], hsend.at[0], hrecv.at[n], (g, c))

    def sems(p, t, i):
        n = (p * NPART + t) * 4 + i
        return gsend.at[n], grecv.at[n]

    def g2(p, t, sign):
        return rdma(qbuf.at[p, t, 0], qbuf.at[p, t, 3 if sign > 0 else 1],
                    *sems(p, t, 0 if sign > 0 else 1), nbr(p, t, sign))

    def g2f(p, t, sign):
        half = pl.ds(0, 2) if sign > 0 else pl.ds(2, 2)
        return rdma(qbuf.at[p, t, 3 if sign > 0 else 1, half], qbuf.at[p, t, 2, half],
                    *sems(p, t, 2 if sign > 0 else 3), nbr(p, t, sign))

    def send1(p, t):
        for d in (1, 3, 2):
            along(p, t, d).start()

    def yget(t, a):
        return rdma(qbuf.at[0, t, a], qbuf.at[1, t, a], *sems(1, t, a), (g, other))

    def send2(p, t):
        for d in range(1, 4):
            along(p, t, d).wait_recv()
        g2(p, t, 1).start()
        g2(p, t, -1).start()
        if (p, t) in early:
            yget(t, 0).start()

    def spread(p, t):
        if t < 3:
            across(t).wait_recv()
        else:
            mine = (g == (t - 3) * 2 + p) & (y == k)
            pl.when(jnp.logical_not(mine))(handed_in(p, t).wait_recv)
        send1(p, t)

    def relay2(p, t):
        for sign in (1, -1):
            g2(p, t, sign).wait_recv()
            g2f(p, t, sign).start()
            if (p, t) in early:
                yget(t, 3 if sign > 0 else 1).start()

    def ready(p, t):
        for sign in (1, -1):
            g2f(p, t, sign).wait_recv()
        if (p, t) in early:
            yget(t, 2).start()

    def yready(*dists):
        for a in dists:
            for _, t in middle:
                yget(t, a).wait_recv()

    early = [(0, 0), (0, 1)]
    middle = [(1, 0), (1, 1)]
    late = [(1, 2), (0, 2)]
    slot_u = [(0, 3), (1, 3), (0, 4), (1, 4)]
    order = early + middle + slot_u + late

    def handed_do(what):
        for hh in range(2):
            for yy in range(2):
                mine = (2 * hh + y == g) & (y == yy)
                cp = handed(hh, yy)
                pl.when(jnp.logical_not(mine))(cp.start if what else cp.wait_send)

    send1(0, 0)
    send1(0, 1)
    across(2).start()
    handed_do(True)
    send1(0, 2)

    @pl.when(y == k)
    def _():
        qbuf[g % 2, 3 + g // 2, 0, 0] = qown[3]

    swap = rdma(cache_ref, cbuf.at[1], csem.at[3], csem.at[4], (g + 1 - 2 * k, c))

    def store(ref, base, o):
        for i in range(4):
            ref[base + i] = o[:, 128 * i:128 * i + 128].astype(BF)

    def load(ref, base):
        return chunk([ref[base + i] for i in range(4)])

    nj = 2
    wj = CTX // nj
    start_pos = c * CTX

    def attend(groups):
        n = len(groups)
        p, t, _ = groups[0]
        if t < 3:
            keys = cbuf.at[0]
            limit = len_ref[g] - start_pos
        else:
            d = don_ref[(t - 3) * 2 + p]
            keys = cbuf.at[jnp.where(d % 2 == k, 0, 1)]
            limit = jnp.where(d // 2 == h, len_ref[d] - start_pos, 0)
        q = jnp.concatenate([qbuf[p, t, a].reshape(64, KEYW) for p, t, a in groups], axis=0)

        def score(j):
            pos = lax.broadcasted_iota(jnp.int32, (1, wj), 1) + j * wj
            bias = jnp.where(pos < limit, 0.0, LOW)
            return jnp.dot(q, keys[:, j * wj:(j + 1) * wj], preferred_element_type=F32) * SCALE2 + bias

        top = total = acc = None
        later = score(0)
        for j in range(nj):
            sc = later
            if j + 1 < nj:
                later = score(j + 1)
            peak = rounded(jnp.maximum(jnp.max(sc, axis=1, keepdims=True), FLOOR if top is None else top))
            w = jnp.exp2(sc - peak)
            part = jnp.sum(w, axis=1, keepdims=True)
            val = lax.dot_general(w.astype(BF), keys[:LATENT, j * wj:(j + 1) * wj],
                                  (((1,), (1,)), ((), ())), preferred_element_type=F32)
            if top is None:
                total, acc = part, val
            else:
                scale = jnp.exp2(top - peak)
                total = total * scale + part
                acc = acc * scale + val
            top = peak
        hi = rounded(total)
        lo = total - hi
        for i, (p, t, a) in enumerate(groups):
            for b in range(4):
                store(obuf.at[p, t, a], TILE[b], acc[64 * i + ROWS * b:64 * i + ROWS * b + ROWS])
            tile = jnp.zeros((ROWS, 128), F32)
            for b in range(4):
                part = slice((i * 4 + b) * ROWS, (i * 4 + b + 1) * ROWS)
                tile = jnp.where(lane == b, top[part], tile)
                tile = jnp.where(lane == 4 + b, hi[part], tile)
                tile = jnp.where(lane == 8 + b, lo[part], tile)
            obuf[p, t, a, STAT] = tile.astype(BF)

    def rsem(p, t, i):
        n = (p * NPART + t) * 4 + i
        return rsend.at[n], rrecv.at[n]

    def a1(p, t, sign):
        i = 0 if sign > 0 else 1
        return rdma(obuf.at[p, t, 2, pl.ds(8 * i, 9)], ra.at[p, t, i], *rsem(p, t, i), nbr(p, t, sign))

    def a2(p, t, sign):
        i = 0 if sign > 0 else 1
        return rdma(obuf.at[p, t, 1 if sign > 0 else 3], rc.at[p, t, i], *rsem(p, t, 2 + i), nbr(p, t, sign))

    def back(p, t, d):
        dz, dx = line(p, t, d)
        if t < 3:
            i = t * 7 + (d - 1 if p == 0 else 3 + d)
            if p == 1 and d == 0:
                return rdma(by.at[t], rd.at[i], dsend.at[i], drecv.at[i], (g, other))
            return rdma(bb.at[p, t, d], rd.at[i], dsend.at[i], drecv.at[i], (g, at(dz, dx, y)))
        s = (t - 3) * 2 + p
        i = (2 * h + y) * 4 + d
        return rdma(bb.at[p, t, d], rf.at[i], fsend.at[s * 4 + d], frecv.at[i], (s, at(dz, dx, k)))

    def only(pair, keep):
        return jnp.where(keep, pair[0], 4 * FLOOR), jnp.where(keep, pair[1], 0.0)

    def shifted(pair, b):
        if b == 0:
            return pair
        return pltpu.roll(pair[0], 128 - b, 1), pltpu.roll(pair[1], 128 - b, 1)

    def begin(p, t):
        a1(p, t, 1).start()
        a1(p, t, -1).start()

    def r1(units):
        for p, t in units:
            a1(p, t, 1).wait_recv()
            a1(p, t, -1).wait_recv()
        for p, t in units:
            for i in range(2):
                own = obuf.at[p, t, 1 if i == 0 else 3]
                came = ra.at[p, t, i]
                inside = (lane < 2) if i == 0 else (lane >= 2) & (lane < 4)
                top, total, (f0, f1) = combine([stats(own[STAT]), only(stats(came[STAT if i == 0 else 0]), inside)])
                for b in (2 * i, 2 * i + 1):
                    o = load(own, TILE[b]) * f0[:, b:b + 1] + load(came, TILE[b] - 8 * i) * f1[:, b:b + 1]
                    store(own, TILE[b], o)
                own[STAT] = packed(top, total)
        for p, t in units:
            a2(p, t, 1).start()
            a2(p, t, -1).start()

    def r2(units):
        for p, t in units:
            a2(p, t, 1).wait_recv()
            a2(p, t, -1).wait_recv()
        for p, t in units:
            refs = [obuf.at[p, t, 0], rc.at[p, t, 0], rc.at[p, t, 1]]
            top, total, fs = combine([stats(r[STAT]) for r in refs])
            tile = packed(top, total)
            for b in range(4):
                o = load(refs[0], TILE[b]) * fs[0][:, b:b + 1]
                for r, f in zip(refs[1:], fs[1:]):
                    o = o + load(r, TILE[b]) * f[:, b:b + 1]
                store(bb.at[p, t, b], 0, o)
                bb[p, t, b, 4] = tile
        for p, t in units:
            for d in (2, 1, 3):
                back(p, t, d).start()
            if t >= 3:
                mine = (g == (t - 3) * 2 + p) & (y == k)
                pl.when(jnp.logical_not(mine))(back(p, t, 0).start)

                @pl.when(mine)
                def _():
                    rf[(2 * h + y) * 4] = bb[p, t, 0]

    def r3(units):
        for p, t in units:
            for d in (1, 2, 3):
                back(p, t, d).wait_recv()
        for p, t in units:
            refs = [rd.at[t * 7 + 3 + d] for d in (1, 2, 3)]
            top, total, fs = combine([stats(bb[p, t, 0, 4])] + [shifted(stats(r[4]), d + 1) for d, r in enumerate(refs)])
            o = load(bb.at[p, t, 0], 0) * fs[0][:, 0:1]
            for r, f in zip(refs, fs[1:]):
                o = o + load(r, 0) * f[:, 0:1]
            store(by.at[t], 0, o)
            by[t, 4] = packed(top, total)
        for p, t in units:
            back(p, t, 0).start()

    att = [None] * 4

    def fold_in(t, parts, outs, last):
        parts = parts + [(fst[t, 0], fst[t, 1])]
        top, total, fs = combine(parts)
        o = fo[t] * fs[-1][:, 0:1]
        for f, v in zip(fs[:-1], outs):
            o = o + load(v, 0) * f[:, 0:1]
        if last:
            att[t] = (o / total[:, 0:1]).astype(BF)
        else:
            fo[t] = o
            fst[t, 0] = top
            fst[t, 1] = total

    def fin_half(p, t):
        ds = (1, 2, 3) if p == 0 else (0,)
        for d in ds:
            back(p, t, d).wait_recv()
        where = [t * 7 + (d - 1 if p == 0 else 3 + d) for d in ds]
        parts = [shifted(stats(rd[i, 4]), d) for i, d in zip(where, ds)]
        outs = [rd.at[i] for i in where]
        if p == 0:
            parts.append(stats(bb[0, t, 0, 4]))
            outs.append(bb.at[0, t, 0])
        fold_in(t, parts, outs, p == 1)

    def fin_slot():
        for i in range(16):
            cp = rdma(bb.at[0, 3, 0], rf.at[i], fsend.at[0], frecv.at[i], (g, c))
            if i % 4 == 0:
                mine = (y == k) & (i // 4 == 2 * h + y)
                pl.when(jnp.logical_not(mine))(cp.wait_recv)
            else:
                cp.wait_recv()
        fold_in(3, [shifted(stats(rf[i, 4]), i % 4) for i in range(16)], [rf.at[i] for i in range(16)], True)

    def each(f, units):
        for u in units:
            f(*u)

    def of(units, *dists):
        return [(p, t, a) for a in dists for p, t in units]

    phase("g1")
    each(send2, early)
    spread(*late[0])
    each(spread, slot_u)
    own_copy.wait()
    phase("B1")
    attend(of(early, 0))
    phase("g2")
    each(relay2, early)
    each(send2, late)
    swap.start()
    phase("B2")
    attend(of(early, 1, 3))
    phase("g3")
    each(send2, slot_u)
    each(ready, early)
    phase("g3y")
    yready(0)
    phase("B3")
    attend(of(early, 2) + of(middle, 0))
    each(begin, early)
    phase("g4")
    each(relay2, late)
    each(relay2, slot_u[:2])
    phase("g4y")
    yready(1, 3)
    phase("B4")
    attend(of(middle, 1, 3))
    phase("g5")
    each(relay2, slot_u[2:])
    swap.wait()

    def slot(i):
        phase("ws%d" % i)
        ready(*slot_u[i])
        phase("S%d" % i)
        attend(of(slot_u[i:i + 1], 0, 1, 2, 3))
        begin(*slot_u[i])
        phase("rs%d" % i)

    slot(0)
    r1(early)
    phase("g6")
    yready(2)
    each(ready, late)
    phase("B5")
    attend(of(middle, 2) + of(late, 2))
    each(begin, middle)
    each(begin, late)
    slot(1)
    r1(slot_u[0:1])
    slot(2)
    r2(early)
    r1(middle)
    slot(3)
    r1(slot_u[1:2])
    phase("M3")
    attend(of(late, 1, 3) + of(late[:1], 0))
    phase("rm3")
    r1(late)
    r2(middle)
    r1(slot_u[2:3])
    r2(slot_u[0:1])
    phase("E")
    attend(of(late[1:], 0))
    phase("re")
    r1(slot_u[3:])
    r2(slot_u[1:2])
    phase("rlate")
    r2(late)
    phase("rmid")
    r3(middle)
    fin_half(0, 0)
    fin_half(0, 1)
    phase("rs12")
    r2(slot_u[2:3])
    phase("rl3")
    r3(late[:1])
    phase("rs13")
    r2(slot_u[3:])
    phase("f1")
    fin_half(1, 0)
    fin_half(1, 1)
    fin_half(0, 2)
    phase("f2")
    fin_half(1, 2)
    phase("fs")
    fin_slot()

    phase("tail")
    attended = jnp.concatenate(att, axis=0)
    vu_copy.wait()
    op_copy.wait()
    row_head = lax.broadcasted_iota(jnp.int32, (64, 128), 0) % 4
    pieces = []
    for head in range(4):
        hv = jnp.dot(attended, vuv[head], preferred_element_type=F32)
        pieces.append(jnp.where(row_head == head, hv, 0.0).astype(BF))
    spread = jnp.concatenate(pieces, axis=1)
    pick = (lax.broadcasted_iota(jnp.int32, (ROWS, 64), 1) // 4
            == lax.broadcasted_iota(jnp.int32, (ROWS, 64), 0))
    joined = jnp.dot(jnp.where(pick, 1.0, 0.0).astype(BF), spread, preferred_element_type=F32).astype(BF)

    def outc(dest, rel):
        return rdma(sbuf.at[dest], rbuf.at[rel], xsend.at[dest], xrecv.at[rel], (g, dest))

    width = 8 * OUTW
    for blk in range(4):
        term = jnp.dot(joined, opv[:, blk * width:(blk + 1) * width], preferred_element_type=F32)
        for i in range(8):
            dest = blk * 8 + i
            sbuf[dest, :, :OUTW] = term[:, i * OUTW:(i + 1) * OUTW].astype(BF)
        for i in range(8):
            dest = blk * 8 + i
            pl.when(dest != c)(outc(dest, (c - dest + NPEER) % NPEER).start)
    phase("outx")

    handed_do(False)
    for p, t in order:
        for d in (1, 2, 3):
            if (p, t) not in middle:
                along(p, t, d).wait_send()
            back(p, t, d).wait_send()
        if t >= 3:
            mine = (g == (t - 3) * 2 + p) & (y == k)
            pl.when(jnp.logical_not(mine))(back(p, t, 0).wait_send)
        elif p == 1:
            back(p, t, 0).wait_send()
            if (p, t) in middle:
                for a in range(4):
                    yget(t, a).wait_send()
            else:
                across(t).wait_send()
        for sign in (1, -1):
            if (p, t) not in middle:
                g2(p, t, sign).wait_send()
                g2f(p, t, sign).wait_send()
            a1(p, t, sign).wait_send()
            a2(p, t, sign).wait_send()

    res = sbuf[c][:, :OUTW].astype(F32)
    for rel in range(1, NPEER):
        pltpu.make_async_remote_copy(src_ref=sbuf.at[0], dst_ref=rbuf.at[rel], send_sem=xsend.at[0],
                                     recv_sem=xrecv.at[rel], device_id=(g, c), device_id_type=MESH).wait_recv()
        res = res + rbuf[rel][:, :OUTW].astype(F32)
    for t in range(4):
        out_ref[t, 0] = res[4 * t:4 * t + 4].astype(BF)

    def sent_out(i, carry):
        outc((c + i) % NPEER, (NPEER - i) % NPEER).wait_send()
        return carry

    lax.fori_loop(1, NPEER, sent_out, 0)
    phase(None)


def body(cache, queries, new_latent, lengths, donor, value_up, out_proj):
    keys = jnp.swapaxes(cache[0], 0, 1)
    VM, SM, ANY = pltpu.VMEM, pltpu.SMEM, pl.ANY
    U = (2, NPART)
    dma = pltpu.SemaphoreType.DMA
    return pl.pallas_call(
        kernel,
        out_shape=jax.ShapeDtypeStruct((4, 1, 4, OUTW), BF),
        in_specs=[pl.BlockSpec(memory_space=m) for m in (SM, SM, VM, VM, ANY, ANY, ANY)],
        out_specs=pl.BlockSpec(memory_space=VM),
        scratch_shapes=[
            VM((2, KEYW, CTX), BF),
            VM((4, ROWS, KEYW), BF),
            VM(U + (4, 4, ROWS, KEYW), BF),
            VM(U + (4, 17, ROWS, 128), BF),
            VM(U + (2, 9, ROWS, 128), BF),
            VM(U + (2, 17, ROWS, 128), BF),
            VM(U + (4, 5, ROWS, 128), BF),
            VM((3, 5, ROWS, 128), BF),
            VM((21, 5, ROWS, 128), BF),
            VM((16, 5, ROWS, 128), BF),
            VM((NPEER, ROWS, 256), BF), VM((NPEER, ROWS, 256), BF),
            VM((512, 7168), BF), VM((4, LATENT, 128), BF),
            VM((4, ROWS, LATENT), F32), VM((4, 2, ROWS, 128), F32),
            dma((5,)), dma((44,)), dma((40,)), dma((40,)), dma((40,)), dma((40,)), dma((40,)),
            dma((NPEER,)), dma((NPEER,)), dma((21,)), dma((21,)), dma((16,)), dma((16,)),
        ],
        compiler_params=pltpu.CompilerParams(collective_id=0, has_side_effects=True,
                                             vmem_limit_bytes=56 * 1024 * 1024),
        name="mla_step",
    )(lengths, donor, queries, new_latent, keys, value_up, out_proj)


def solution(mesh):
    return jax.shard_map(
        body,
        mesh=mesh,
        in_specs=(
            P("grp", "ctx", None),
            P(None, "grp", None, "ctx", None),
            P(None, "grp", None, None),
            P(),
            P(),
            P("ctx", None, None),
            P("ctx", None),
        ),
        out_specs=P(None, "grp", None, "ctx"),
        check_vma=False,
    )
```

```python
import functools

import jax
import jax.numpy as jnp
from jax import lax
from jax.experimental import pallas as pl
from jax.experimental.pallas import tpu as pltpu
from jax.sharding import PartitionSpec as P

MESH = pl.DeviceIdType.MESH
LATENT = 512
KEYW = 576
CTX = 2048
ROWS = 16
UNIT = 256
NPART = 5
OUTW = 224
NPEER = 32
SCALE2 = (192.0 ** -0.5) * 1.4426950408889634
LOW = -1e30
FLOOR = -1e29
BF = jnp.bfloat16
F32 = jnp.float32
XLINE = ((0, 0), (1, 0), (0, 2), (1, 3), (0, 4))


def rounded(v):
    return v.astype(BF).astype(F32)


def lanes_of(shape):
    return lax.broadcasted_iota(jnp.int32, shape, 1)


def stats(tile):
    t = tile.astype(F32)
    return t, pltpu.roll(t, 124, 1) + pltpu.roll(t, 120, 1)


TILE = (0, 4, 9, 13)
STAT = 8


def chunk(tiles):
    return jnp.concatenate(tiles, axis=1).astype(F32)


def combine(parts):
    top = parts[0][0]
    for t, _ in parts[1:]:
        top = jnp.maximum(top, t)
    factors = [jnp.exp2(t - top) for t, _ in parts]
    total = factors[0] * parts[0][1]
    for f, (_, v) in zip(factors[1:], parts[1:]):
        total = total + f * v
    return top, total, factors


def packed(top, total):
    lane = lanes_of(top.shape)
    hi = rounded(total)
    lo = total - hi
    return jnp.where(lane < 4, top, jnp.where(lane < 8, pltpu.roll(hi, 4, 1), pltpu.roll(lo, 8, 1))).astype(BF)


def kernel(len_ref, don_ref, q_ref, nl_ref, cache_ref, vu_ref, op_ref, out_ref,
           cbuf, qown, qbuf, obuf, ra, rc, bb, by, rd, rf, sbuf, rbuf, opv, vuv, fo, fst,
           csem, hsend, hrecv, gsend, grecv, rsend, rrecv, xsend, xrecv, dsend, drecv, fsend, frecv):
    g = lax.axis_index("grp")
    c = lax.axis_index("ctx")
    h = g // 2
    k = g % 2
    z = c // 8
    x = (c // 2) % 4
    y = c % 2
    other = c + 1 - 2 * y

    def at(dz, dx, yy):
        return ((z + dz + 4) % 4) * 8 + ((x + dx + 4) % 4) * 2 + yy

    def line(p, t, d):
        return (0, d) if (p, t) in XLINE else (d, 0)

    def nbr(p, t, d):
        dx, dz = line(p, t, d)
        return (g, at(dz, dx, y))

    def rdma(src, dst, ss, rs, dev):
        return pltpu.make_async_remote_copy(src_ref=src, dst_ref=dst, send_sem=ss, recv_sem=rs,
                                            device_id=dev, device_id_type=MESH)

    scope = [None]

    def phase(name):
        if scope[0] is not None:
            scope[0].__exit__(None, None, None)
            scope[0] = None
        if name:
            scope[0] = jax.named_scope(name)
            scope[0].__enter__()

    phase("enter")
    barrier = pltpu.get_barrier_semaphore()

    def greet(i, carry):
        pl.semaphore_signal(barrier, inc=1, device_id=(g, (c + i) % NPEER), device_id_type=MESH)
        return carry

    lax.fori_loop(1, NPEER, greet, 0)
    places = [(0, 0)] + [(d, 0) for d in range(1, 4)] + [(0, d) for d in range(1, 4)]
    for dg in range(1, 4):
        for dz, dx in places:
            for yy in range(2):
                pl.semaphore_signal(barrier, inc=1, device_id=((g + dg) % 4, at(dz, dx, yy)), device_id_type=MESH)

    own_copy = pltpu.make_async_copy(cache_ref, cbuf.at[0], csem.at[0])
    own_copy.start()
    vu_copy = pltpu.make_async_copy(vu_ref, vuv, csem.at[2])
    vu_copy.start()
    op_copy = pltpu.make_async_copy(op_ref, opv, csem.at[1])
    op_copy.start()
    for t in range(4):
        for s in range(4):
            qown[t, 4 * s:4 * s + 4] = q_ref[t, 0, s]
    for t in range(3):
        qbuf[0, t, 0, 0] = qown[t]

    lane = lanes_of((ROWS, 128))
    lane_k = lanes_of((ROWS, 4))
    row_s = lax.broadcasted_iota(jnp.int32, (ROWS, 4), 0) // 4
    for t in range(4):
        q = qown[t]
        logits = []
        for u in range(t + 1):
            lg = lax.dot_general(q, nl_ref[u, 0], (((1,), (1,)), ((), ())), preferred_element_type=F32)
            logits.append(jnp.where(lane_k == row_s, lg * SCALE2, LOW))
        top = jnp.max(logits[0], axis=1, keepdims=True)
        for lg in logits[1:]:
            top = jnp.maximum(top, jnp.max(lg, axis=1, keepdims=True))
        total = jnp.zeros((ROWS, 1), F32)
        acc = jnp.zeros((ROWS, LATENT), F32)
        for u in range(t + 1):
            w = jnp.where(lane_k == row_s, jnp.exp2(logits[u] - top), 0.0)
            total = total + jnp.sum(w, axis=1, keepdims=True)
            val = nl_ref[u, 0][:, :LATENT]
            whi = w.astype(BF)
            wlo = (w - whi.astype(F32)).astype(BF)
            acc = acc + (jnp.dot(whi, val, preferred_element_type=F32)
                         + jnp.dot(wlo, val, preferred_element_type=F32))
        fo[t] = acc
        fst[t, 0] = jnp.broadcast_to(top, (ROWS, 128))
        fst[t, 1] = jnp.broadcast_to(total, (ROWS, 128))

    pl.semaphore_wait(barrier, NPEER - 1 + 42)
    phase("prep")

    def hsems(p, t, d):
        n = (p * NPART + t) * 4 + d
        return hsend.at[n], hrecv.at[n]

    def along(p, t, d):
        dz, dx = line(p, t, d)
        return rdma(qbuf.at[p, t, 0, 0], qbuf.at[p, t, 0, (4 - d) % 4], *hsems(p, t, d), (g, at(dz, dx, y)))

    def across(t):
        return rdma(qown.at[t], qbuf.at[1, t, 0, 0], *hsems(1, t, 0), (g, other))

    def handed(hh, yy):
        n = ((g % 2) * NPART + 3 + g // 2) * 4
        return rdma(qown.at[3], qbuf.at[g % 2, 3 + g // 2, 0, 0],
                    hsend.at[40 + 2 * hh + yy], hrecv.at[n], (2 * hh + y, at(0, 0, yy)))

    def handed_in(p, t):
        n = (p * NPART + t) * 4
        return rdma(qown.at[3], qbuf.at[p, t, 0, 0], hsend.at[0], hrecv.at[n], (g, c))

    def sems(p, t, i):
        n = (p * NPART + t) * 4 + i
        return gsend.at[n], grecv.at[n]

    def g2(p, t, sign):
        return rdma(qbuf.at[p, t, 0], qbuf.at[p, t, 3 if sign > 0 else 1],
                    *sems(p, t, 0 if sign > 0 else 1), nbr(p, t, sign))

    def g2f(p, t, sign):
        half = pl.ds(0, 2) if sign > 0 else pl.ds(2, 2)
        return rdma(qbuf.at[p, t, 3 if sign > 0 else 1, half], qbuf.at[p, t, 2, half],
                    *sems(p, t, 2 if sign > 0 else 3), nbr(p, t, sign))

    def send1(p, t):
        for d in (1, 3, 2):
            along(p, t, d).start()

    def yget(t, a):
        return rdma(qbuf.at[0, t, a], qbuf.at[1, t, a], *sems(1, t, a), (g, other))

    def send2(p, t):
        for d in range(1, 4):
            along(p, t, d).wait_recv()
        g2(p, t, 1).start()
        g2(p, t, -1).start()
        if (p, t) in early:
            yget(t, 0).start()

    def spread(p, t):
        if t < 3:
            across(t).wait_recv()
        else:
            mine = (g == (t - 3) * 2 + p) & (y == k)
            pl.when(jnp.logical_not(mine))(handed_in(p, t).wait_recv)
        send1(p, t)

    def relay2(p, t):
        for sign in (1, -1):
            g2(p, t, sign).wait_recv()
            g2f(p, t, sign).start()
            if (p, t) in early:
                yget(t, 3 if sign > 0 else 1).start()

    def ready(p, t):
        for sign in (1, -1):
            g2f(p, t, sign).wait_recv()
        if (p, t) in early:
            yget(t, 2).start()

    def yready(*dists):
        for a in dists:
            for _, t in middle:
                yget(t, a).wait_recv()

    early = [(0, 0), (0, 1)]
    middle = [(1, 0), (1, 1)]
    late = [(1, 2), (0, 2)]
    slot_u = [(0, 3), (1, 3), (0, 4), (1, 4)]
    order = early + middle + slot_u + late

    def handed_do(what):
        for hh in range(2):
            for yy in range(2):
                mine = (2 * hh + y == g) & (y == yy)
                cp = handed(hh, yy)
                pl.when(jnp.logical_not(mine))(cp.start if what else cp.wait_send)

    send1(0, 0)
    send1(0, 1)
    across(2).start()
    handed_do(True)
    send1(0, 2)

    @pl.when(y == k)
    def _():
        qbuf[g % 2, 3 + g // 2, 0, 0] = qown[3]

    swap = rdma(cache_ref, cbuf.at[1], csem.at[3], csem.at[4], (g + 1 - 2 * k, c))

    def store(ref, base, o):
        for i in range(4):
            ref[base + i] = o[:, 128 * i:128 * i + 128].astype(BF)

    def load(ref, base):
        return chunk([ref[base + i] for i in range(4)])

    nj = 2
    wj = CTX // nj
    start_pos = c * CTX

    def attend(groups):
        n = len(groups)
        p, t, _ = groups[0]
        if t < 3:
            keys = cbuf.at[0]
            limit = len_ref[g] - start_pos
        else:
            d = don_ref[(t - 3) * 2 + p]
            keys = cbuf.at[jnp.where(d % 2 == k, 0, 1)]
            limit = jnp.where(d // 2 == h, len_ref[d] - start_pos, 0)
        q = jnp.concatenate([qbuf[p, t, a].reshape(64, KEYW) for p, t, a in groups], axis=0)

        def score(j):
            pos = lax.broadcasted_iota(jnp.int32, (1, wj), 1) + j * wj
            bias = jnp.where(pos < limit, 0.0, LOW)
            return jnp.dot(q, keys[:, j * wj:(j + 1) * wj], preferred_element_type=F32) * SCALE2 + bias

        top = total = acc = None
        later = score(0)
        for j in range(nj):
            sc = later
            if j + 1 < nj:
                later = score(j + 1)
            peak = rounded(jnp.maximum(jnp.max(sc, axis=1, keepdims=True), FLOOR if top is None else top))
            w = jnp.exp2(sc - peak)
            part = jnp.sum(w, axis=1, keepdims=True)
            val = lax.dot_general(w.astype(BF), keys[:LATENT, j * wj:(j + 1) * wj],
                                  (((1,), (1,)), ((), ())), preferred_element_type=F32)
            if top is None:
                total, acc = part, val
            else:
                scale = jnp.exp2(top - peak)
                total = total * scale + part
                acc = acc * scale + val
            top = peak
        hi = rounded(total)
        lo = total - hi
        for i, (p, t, a) in enumerate(groups):
            for b in range(4):
                store(obuf.at[p, t, a], TILE[b], acc[64 * i + ROWS * b:64 * i + ROWS * b + ROWS])
            tile = jnp.zeros((ROWS, 128), F32)
            for b in range(4):
                part = slice((i * 4 + b) * ROWS, (i * 4 + b + 1) * ROWS)
                tile = jnp.where(lane == b, top[part], tile)
                tile = jnp.where(lane == 4 + b, hi[part], tile)
                tile = jnp.where(lane == 8 + b, lo[part], tile)
            obuf[p, t, a, STAT] = tile.astype(BF)

    def rsem(p, t, i):
        n = (p * NPART + t) * 4 + i
        return rsend.at[n], rrecv.at[n]

    def a1(p, t, sign):
        i = 0 if sign > 0 else 1
        return rdma(obuf.at[p, t, 2, pl.ds(8 * i, 9)], ra.at[p, t, i], *rsem(p, t, i), nbr(p, t, sign))

    def a2(p, t, sign):
        i = 0 if sign > 0 else 1
        return rdma(obuf.at[p, t, 1 if sign > 0 else 3], rc.at[p, t, i], *rsem(p, t, 2 + i), nbr(p, t, sign))

    def back(p, t, d):
        dz, dx = line(p, t, d)
        if t < 3:
            i = t * 7 + (d - 1 if p == 0 else 3 + d)
            if (p, t) in middle and d == 0:
                return rdma(by.at[t], rd.at[i], dsend.at[i], drecv.at[i], (g, other))
            home = y if p == 0 or (p, t) in middle else 1 - y
            return rdma(bb.at[p, t, d], rd.at[i], dsend.at[i], drecv.at[i], (g, at(dz, dx, home)))
        s = (t - 3) * 2 + p
        i = (2 * h + y) * 4 + d
        return rdma(bb.at[p, t, d], rf.at[i], fsend.at[s * 4 + d], frecv.at[i], (s, at(dz, dx, k)))

    def only(pair, keep):
        return jnp.where(keep, pair[0], 4 * FLOOR), jnp.where(keep, pair[1], 0.0)

    def shifted(pair, b):
        if b == 0:
            return pair
        return pltpu.roll(pair[0], 128 - b, 1), pltpu.roll(pair[1], 128 - b, 1)

    def begin(p, t):
        a1(p, t, 1).start()
        a1(p, t, -1).start()

    def r1(units):
        for p, t in units:
            a1(p, t, 1).wait_recv()
            a1(p, t, -1).wait_recv()
        for p, t in units:
            for i in range(2):
                own = obuf.at[p, t, 1 if i == 0 else 3]
                came = ra.at[p, t, i]
                inside = (lane < 2) if i == 0 else (lane >= 2) & (lane < 4)
                top, total, (f0, f1) = combine([stats(own[STAT]), only(stats(came[STAT if i == 0 else 0]), inside)])
                for b in (2 * i, 2 * i + 1):
                    o = load(own, TILE[b]) * f0[:, b:b + 1] + load(came, TILE[b] - 8 * i) * f1[:, b:b + 1]
                    store(own, TILE[b], o)
                own[STAT] = packed(top, total)
        for p, t in units:
            a2(p, t, 1).start()
            a2(p, t, -1).start()

    def r2(units):
        for p, t in units:
            a2(p, t, 1).wait_recv()
            a2(p, t, -1).wait_recv()
        for p, t in units:
            refs = [obuf.at[p, t, 0], rc.at[p, t, 0], rc.at[p, t, 1]]
            top, total, fs = combine([stats(r[STAT]) for r in refs])
            tile = packed(top, total)
            for b in range(4):
                o = load(refs[0], TILE[b]) * fs[0][:, b:b + 1]
                for r, f in zip(refs[1:], fs[1:]):
                    o = o + load(r, TILE[b]) * f[:, b:b + 1]
                store(bb.at[p, t, b], 0, o)
                bb[p, t, b, 4] = tile
        for p, t in units:
            for d in (2, 1, 3):
                back(p, t, d).start()
            if (p, t) in late[:1]:
                back(p, t, 0).start()
            if t >= 3:
                mine = (g == (t - 3) * 2 + p) & (y == k)
                pl.when(jnp.logical_not(mine))(back(p, t, 0).start)

                @pl.when(mine)
                def _():
                    rf[(2 * h + y) * 4] = bb[p, t, 0]

    def r3(units):
        for p, t in units:
            for d in (1, 2, 3):
                back(p, t, d).wait_recv()
        for p, t in units:
            refs = [rd.at[t * 7 + 3 + d] for d in (1, 2, 3)]
            top, total, fs = combine([stats(bb[p, t, 0, 4])] + [shifted(stats(r[4]), d + 1) for d, r in enumerate(refs)])
            o = load(bb.at[p, t, 0], 0) * fs[0][:, 0:1]
            for r, f in zip(refs, fs[1:]):
                o = o + load(r, 0) * f[:, 0:1]
            store(by.at[t], 0, o)
            by[t, 4] = packed(top, total)
        for p, t in units:
            back(p, t, 0).start()

    att = [None] * 4

    def fold_in(t, parts, outs, last):
        parts = parts + [(fst[t, 0], fst[t, 1])]
        top, total, fs = combine(parts)
        o = fo[t] * fs[-1][:, 0:1]
        for f, v in zip(fs[:-1], outs):
            o = o + load(v, 0) * f[:, 0:1]
        if last:
            att[t] = (o / total[:, 0:1]).astype(BF)
        else:
            fo[t] = o
            fst[t, 0] = top
            fst[t, 1] = total

    def fin_half(p, t):
        ds = (1, 2, 3) if p == 0 else (0,) if (p, t) in middle else (0, 1, 2, 3)
        for d in ds:
            back(p, t, d).wait_recv()
        where = [t * 7 + (d - 1 if p == 0 else 3 + d) for d in ds]
        parts = [shifted(stats(rd[i, 4]), d) for i, d in zip(where, ds)]
        outs = [rd.at[i] for i in where]
        if p == 0:
            parts.append(stats(bb[0, t, 0, 4]))
            outs.append(bb.at[0, t, 0])
        fold_in(t, parts, outs, p == 1)

    def fin_slot():
        for i in range(16):
            cp = rdma(bb.at[0, 3, 0], rf.at[i], fsend.at[0], frecv.at[i], (g, c))
            if i % 4 == 0:
                mine = (y == k) & (i // 4 == 2 * h + y)
                pl.when(jnp.logical_not(mine))(cp.wait_recv)
            else:
                cp.wait_recv()
        fold_in(3, [shifted(stats(rf[i, 4]), i % 4) for i in range(16)], [rf.at[i] for i in range(16)], True)

    def each(f, units):
        for u in units:
            f(*u)

    def of(units, *dists):
        return [(p, t, a) for a in dists for p, t in units]

    phase("g1")
    each(send2, early)
    spread(*late[0])
    each(spread, slot_u)
    own_copy.wait()
    phase("B1")
    attend(of(early, 0))
    phase("g2")
    each(relay2, early)
    each(send2, late)
    swap.start()
    phase("B2")
    attend(of(early, 1, 3))
    phase("g3")
    each(send2, slot_u)
    each(ready, early)
    phase("g3y")
    yready(0)
    phase("B3")
    attend(of(early, 2) + of(middle, 0))
    each(begin, early)
    phase("g4")
    each(relay2, late)
    each(relay2, slot_u[:2])
    phase("g4y")
    yready(1, 3)
    phase("B4")
    attend(of(middle, 1, 3))
    phase("g5")
    each(relay2, slot_u[2:])
    swap.wait()

    def slot(i):
        phase("ws%d" % i)
        ready(*slot_u[i])
        phase("S%d" % i)
        attend(of(slot_u[i:i + 1], 0, 1, 2, 3))
        begin(*slot_u[i])
        phase("rs%d" % i)

    slot(0)
    r1(early)
    phase("g6")
    yready(2)
    each(ready, late)
    phase("B5")
    attend(of(middle, 2) + of(late, 2))
    each(begin, middle)
    each(begin, late)
    slot(1)
    slot(2)
    r1(middle)
    r1(slot_u[0:1])
    slot(3)
    r1(slot_u[1:2])
    phase("M3")
    attend(of(late, 1, 3))
    phase("rm3")
    r1(late)
    r1(slot_u[2:3])
    r2(middle)
    phase("E")
    attend(of(late, 0))
    phase("re")
    r1(slot_u[3:])
    r2(slot_u[0:2])
    phase("rlate")
    r2(late)
    phase("rmid")
    r3(middle)
    r2(early)
    phase("rs12")
    r2(slot_u[2:3])
    phase("rs13")
    r2(slot_u[3:])
    phase("f0")
    fin_half(0, 0)
    fin_half(0, 1)
    phase("f1")
    fin_half(0, 2)
    fin_half(1, 0)
    fin_half(1, 1)
    phase("f2")
    fin_half(1, 2)
    phase("fs")
    fin_slot()

    phase("tail")
    attended = jnp.concatenate(att, axis=0)
    vu_copy.wait()
    op_copy.wait()
    row_head = lax.broadcasted_iota(jnp.int32, (64, 128), 0) % 4
    pieces = []
    for head in range(4):
        hv = jnp.dot(attended, vuv[head], preferred_element_type=F32)
        pieces.append(jnp.where(row_head == head, hv, 0.0).astype(BF))
    spread = jnp.concatenate(pieces, axis=1)
    pick = (lax.broadcasted_iota(jnp.int32, (ROWS, 64), 1) // 4
            == lax.broadcasted_iota(jnp.int32, (ROWS, 64), 0))
    joined = jnp.dot(jnp.where(pick, 1.0, 0.0).astype(BF), spread, preferred_element_type=F32).astype(BF)

    def outc(dest, rel):
        return rdma(sbuf.at[dest], rbuf.at[rel], xsend.at[dest], xrecv.at[rel], (g, dest))

    width = 8 * OUTW
    for blk in range(4):
        term = jnp.dot(joined, opv[:, blk * width:(blk + 1) * width], preferred_element_type=F32)
        for i in range(8):
            dest = blk * 8 + i
            sbuf[dest, :, :OUTW] = term[:, i * OUTW:(i + 1) * OUTW].astype(BF)
        for i in range(8):
            dest = blk * 8 + i
            pl.when(dest != c)(outc(dest, (c - dest + NPEER) % NPEER).start)
    phase("outx")

    handed_do(False)
    for p, t in order:
        for d in (1, 2, 3):
            if (p, t) not in middle:
                along(p, t, d).wait_send()
            back(p, t, d).wait_send()
        if t >= 3:
            mine = (g == (t - 3) * 2 + p) & (y == k)
            pl.when(jnp.logical_not(mine))(back(p, t, 0).wait_send)
        elif p == 1:
            back(p, t, 0).wait_send()
            if (p, t) in middle:
                for a in range(4):
                    yget(t, a).wait_send()
            else:
                across(t).wait_send()
        for sign in (1, -1):
            if (p, t) not in middle:
                g2(p, t, sign).wait_send()
                g2f(p, t, sign).wait_send()
            a1(p, t, sign).wait_send()
            a2(p, t, sign).wait_send()

    res = sbuf[c][:, :OUTW].astype(F32)
    for rel in range(1, NPEER):
        pltpu.make_async_remote_copy(src_ref=sbuf.at[0], dst_ref=rbuf.at[rel], send_sem=xsend.at[0],
                                     recv_sem=xrecv.at[rel], device_id=(g, c), device_id_type=MESH).wait_recv()
        res = res + rbuf[rel][:, :OUTW].astype(F32)
    for t in range(4):
        out_ref[t, 0] = res[4 * t:4 * t + 4].astype(BF)

    def sent_out(i, carry):
        outc((c + i) % NPEER, (NPEER - i) % NPEER).wait_send()
        return carry

    lax.fori_loop(1, NPEER, sent_out, 0)
    phase(None)


def body(cache, queries, new_latent, lengths, donor, value_up, out_proj):
    keys = jnp.swapaxes(cache[0], 0, 1)
    VM, SM, ANY = pltpu.VMEM, pltpu.SMEM, pl.ANY
    U = (2, NPART)
    dma = pltpu.SemaphoreType.DMA
    return pl.pallas_call(
        kernel,
        out_shape=jax.ShapeDtypeStruct((4, 1, 4, OUTW), BF),
        in_specs=[pl.BlockSpec(memory_space=m) for m in (SM, SM, VM, VM, ANY, ANY, ANY)],
        out_specs=pl.BlockSpec(memory_space=VM),
        scratch_shapes=[
            VM((2, KEYW, CTX), BF),
            VM((4, ROWS, KEYW), BF),
            VM(U + (4, 4, ROWS, KEYW), BF),
            VM(U + (4, 17, ROWS, 128), BF),
            VM(U + (2, 9, ROWS, 128), BF),
            VM(U + (2, 17, ROWS, 128), BF),
            VM(U + (4, 5, ROWS, 128), BF),
            VM((2, 5, ROWS, 128), BF),
            VM((21, 5, ROWS, 128), BF),
            VM((16, 5, ROWS, 128), BF),
            VM((NPEER, ROWS, 256), BF), VM((NPEER, ROWS, 256), BF),
            VM((512, 7168), BF), VM((4, LATENT, 128), BF),
            VM((4, ROWS, LATENT), F32), VM((4, 2, ROWS, 128), F32),
            dma((5,)), dma((44,)), dma((40,)), dma((40,)), dma((40,)), dma((40,)), dma((40,)),
            dma((NPEER,)), dma((NPEER,)), dma((21,)), dma((21,)), dma((16,)), dma((16,)),
        ],
        compiler_params=pltpu.CompilerParams(collective_id=0, has_side_effects=True,
                                             vmem_limit_bytes=56 * 1024 * 1024),
        name="mla_step",
    )(lengths, donor, queries, new_latent, keys, value_up, out_proj)


def solution(mesh):
    return jax.shard_map(
        body,
        mesh=mesh,
        in_specs=(
            P("grp", "ctx", None),
            P(None, "grp", None, "ctx", None),
            P(None, "grp", None, None),
            P(),
            P(),
            P("ctx", None, None),
            P("ctx", None),
        ),
        out_specs=P(None, "grp", None, "ctx"),
        check_vma=False,
    )
```

```python
import functools

import jax
import jax.numpy as jnp
from jax import lax
from jax.experimental import pallas as pl
from jax.experimental.pallas import tpu as pltpu
from jax.sharding import PartitionSpec as P

MESH = pl.DeviceIdType.MESH
LATENT = 512
KEYW = 576
CTX = 2048
ROWS = 16
UNIT = 256
NPART = 5
OUTW = 224
NPEER = 32
SCALE2 = (192.0 ** -0.5) * 1.4426950408889634
LOW = -1e30
FLOOR = -1e29
BF = jnp.bfloat16
F32 = jnp.float32
XLINE = ((0, 0), (1, 0), (0, 2), (1, 3), (0, 4))


def rounded(v):
    return v.astype(BF).astype(F32)


def lanes_of(shape):
    return lax.broadcasted_iota(jnp.int32, shape, 1)


def stats(tile):
    t = tile.astype(F32)
    return t, pltpu.roll(t, 124, 1) + pltpu.roll(t, 120, 1)


TILE = (0, 4, 9, 13)
STAT = 8


def chunk(tiles):
    return jnp.concatenate(tiles, axis=1).astype(F32)


def combine(parts):
    top = parts[0][0]
    for t, _ in parts[1:]:
        top = jnp.maximum(top, t)
    factors = [jnp.exp2(t - top) for t, _ in parts]
    total = factors[0] * parts[0][1]
    for f, (_, v) in zip(factors[1:], parts[1:]):
        total = total + f * v
    return top, total, factors


def packed(top, total):
    lane = lanes_of(top.shape)
    hi = rounded(total)
    lo = total - hi
    return jnp.where(lane < 4, top, jnp.where(lane < 8, pltpu.roll(hi, 4, 1), pltpu.roll(lo, 8, 1))).astype(BF)


def kernel(len_ref, don_ref, q_ref, nl_ref, cache_ref, vu_ref, op_ref, out_ref,
           cbuf, qown, qbuf, obuf, ra, rc, bb, by, rd, rf, sbuf, rbuf, opv, vuv, fo, fst,
           csem, hsend, hrecv, gsend, grecv, rsend, rrecv, xsend, xrecv, dsend, drecv, fsend, frecv):
    g = lax.axis_index("grp")
    c = lax.axis_index("ctx")
    h = g // 2
    k = g % 2
    z = c // 8
    x = (c // 2) % 4
    y = c % 2
    other = c + 1 - 2 * y

    def at(dz, dx, yy):
        return ((z + dz + 4) % 4) * 8 + ((x + dx + 4) % 4) * 2 + yy

    def line(p, t, d):
        return (0, d) if (p, t) in XLINE else (d, 0)

    def nbr(p, t, d):
        dx, dz = line(p, t, d)
        return (g, at(dz, dx, y))

    def rdma(src, dst, ss, rs, dev):
        return pltpu.make_async_remote_copy(src_ref=src, dst_ref=dst, send_sem=ss, recv_sem=rs,
                                            device_id=dev, device_id_type=MESH)

    scope = [None]

    def phase(name):
        if scope[0] is not None:
            scope[0].__exit__(None, None, None)
            scope[0] = None
        if name:
            scope[0] = jax.named_scope(name)
            scope[0].__enter__()

    phase("enter")
    barrier = pltpu.get_barrier_semaphore()

    def greet(i, carry):
        pl.semaphore_signal(barrier, inc=1, device_id=(g, (c + i) % NPEER), device_id_type=MESH)
        return carry

    lax.fori_loop(1, NPEER, greet, 0)
    places = [(0, 0)] + [(d, 0) for d in range(1, 4)] + [(0, d) for d in range(1, 4)]
    for dg in range(1, 4):
        for dz, dx in places:
            for yy in range(2):
                pl.semaphore_signal(barrier, inc=1, device_id=((g + dg) % 4, at(dz, dx, yy)), device_id_type=MESH)

    own_copy = pltpu.make_async_copy(cache_ref, cbuf.at[0], csem.at[0])
    own_copy.start()
    vu_copy = pltpu.make_async_copy(vu_ref, vuv, csem.at[2])
    vu_copy.start()
    op_copy = pltpu.make_async_copy(op_ref, opv, csem.at[1])
    op_copy.start()
    for t in range(4):
        for s in range(4):
            qown[t, 4 * s:4 * s + 4] = q_ref[t, 0, s]
    for t in range(3):
        qbuf[0, t, 0, 0] = qown[t]

    lane = lanes_of((ROWS, 128))
    lane_k = lanes_of((ROWS, 4))
    row_s = lax.broadcasted_iota(jnp.int32, (ROWS, 4), 0) // 4
    for t in range(4):
        q = qown[t]
        logits = []
        for u in range(t + 1):
            lg = lax.dot_general(q, nl_ref[u, 0], (((1,), (1,)), ((), ())), preferred_element_type=F32)
            logits.append(jnp.where(lane_k == row_s, lg * SCALE2, LOW))
        top = jnp.max(logits[0], axis=1, keepdims=True)
        for lg in logits[1:]:
            top = jnp.maximum(top, jnp.max(lg, axis=1, keepdims=True))
        total = jnp.zeros((ROWS, 1), F32)
        acc = jnp.zeros((ROWS, LATENT), F32)
        for u in range(t + 1):
            w = jnp.where(lane_k == row_s, jnp.exp2(logits[u] - top), 0.0)
            total = total + jnp.sum(w, axis=1, keepdims=True)
            val = nl_ref[u, 0][:, :LATENT]
            whi = w.astype(BF)
            wlo = (w - whi.astype(F32)).astype(BF)
            acc = acc + (jnp.dot(whi, val, preferred_element_type=F32)
                         + jnp.dot(wlo, val, preferred_element_type=F32))
        fo[t] = acc
        fst[t, 0] = jnp.broadcast_to(top, (ROWS, 128))
        fst[t, 1] = jnp.broadcast_to(total, (ROWS, 128))

    pl.semaphore_wait(barrier, NPEER - 1 + 42)
    phase("prep")

    def hsems(p, t, d):
        n = (p * NPART + t) * 4 + d
        return hsend.at[n], hrecv.at[n]

    def along(p, t, d):
        dz, dx = line(p, t, d)
        return rdma(qbuf.at[p, t, 0, 0], qbuf.at[p, t, 0, (4 - d) % 4], *hsems(p, t, d), (g, at(dz, dx, y)))

    def across(t):
        return rdma(qown.at[t], qbuf.at[1, t, 0, 0], *hsems(1, t, 0), (g, other))

    def handed(hh, yy):
        n = ((g % 2) * NPART + 3 + g // 2) * 4
        return rdma(qown.at[3], qbuf.at[g % 2, 3 + g // 2, 0, 0],
                    hsend.at[40 + 2 * hh + yy], hrecv.at[n], (2 * hh + y, at(0, 0, yy)))

    def handed_in(p, t):
        n = (p * NPART + t) * 4
        return rdma(qown.at[3], qbuf.at[p, t, 0, 0], hsend.at[0], hrecv.at[n], (g, c))

    def sems(p, t, i):
        n = (p * NPART + t) * 4 + i
        return gsend.at[n], grecv.at[n]

    def g2(p, t, sign):
        return rdma(qbuf.at[p, t, 0], qbuf.at[p, t, 3 if sign > 0 else 1],
                    *sems(p, t, 0 if sign > 0 else 1), nbr(p, t, sign))

    def g2f(p, t, sign):
        half = pl.ds(0, 2) if sign > 0 else pl.ds(2, 2)
        return rdma(qbuf.at[p, t, 3 if sign > 0 else 1, half], qbuf.at[p, t, 2, half],
                    *sems(p, t, 2 if sign > 0 else 3), nbr(p, t, sign))

    def send1(p, t):
        for d in (1, 3, 2):
            along(p, t, d).start()

    def yget(t, a):
        return rdma(qbuf.at[0, t, a], qbuf.at[1, t, a], *sems(1, t, a), (g, other))

    def send2(p, t):
        for d in range(1, 4):
            along(p, t, d).wait_recv()
        g2(p, t, 1).start()
        g2(p, t, -1).start()
        if (p, t) in early:
            yget(t, 0).start()

    def spread(p, t):
        if t < 3:
            across(t).wait_recv()
        else:
            mine = (g == (t - 3) * 2 + p) & (y == k)
            pl.when(jnp.logical_not(mine))(handed_in(p, t).wait_recv)
        send1(p, t)

    def relay2(p, t):
        for sign in (1, -1):
            g2(p, t, sign).wait_recv()
            g2f(p, t, sign).start()
            if (p, t) in early:
                yget(t, 3 if sign > 0 else 1).start()

    def ready(p, t):
        for sign in (1, -1):
            g2f(p, t, sign).wait_recv()
        if (p, t) in early:
            yget(t, 2).start()

    def yready(*dists):
        for a in dists:
            for _, t in middle:
                yget(t, a).wait_recv()

    early = [(0, 0), (0, 1)]
    middle = [(1, 0), (1, 1)]
    late = [(1, 2), (0, 2)]
    slot_u = [(0, 3), (1, 3), (0, 4), (1, 4)]
    order = early + middle + slot_u + late

    def handed_do(what):
        for hh in range(2):
            for yy in range(2):
                mine = (2 * hh + y == g) & (y == yy)
                cp = handed(hh, yy)
                pl.when(jnp.logical_not(mine))(cp.start if what else cp.wait_send)

    send1(0, 0)
    send1(0, 1)
    across(2).start()
    handed_do(True)
    send1(0, 2)

    @pl.when(y == k)
    def _():
        qbuf[g % 2, 3 + g // 2, 0, 0] = qown[3]

    swap = rdma(cache_ref, cbuf.at[1], csem.at[3], csem.at[4], (g + 1 - 2 * k, c))

    def store(ref, base, o):
        for i in range(4):
            ref[base + i] = o[:, 128 * i:128 * i + 128].astype(BF)

    def load(ref, base):
        return chunk([ref[base + i] for i in range(4)])

    nj = 2
    wj = CTX // nj
    start_pos = c * CTX

    def attend(groups):
        n = len(groups)
        p, t, _ = groups[0]
        if t < 3:
            keys = cbuf.at[0]
            limit = len_ref[g] - start_pos
        else:
            d = don_ref[(t - 3) * 2 + p]
            keys = cbuf.at[jnp.where(d % 2 == k, 0, 1)]
            limit = jnp.where(d // 2 == h, len_ref[d] - start_pos, 0)
        q = jnp.concatenate([qbuf[p, t, a].reshape(64, KEYW) for p, t, a in groups], axis=0)

        def score(j):
            pos = lax.broadcasted_iota(jnp.int32, (1, wj), 1) + j * wj
            bias = jnp.where(pos < limit, 0.0, LOW)
            return jnp.dot(q, keys[:, j * wj:(j + 1) * wj], preferred_element_type=F32) * SCALE2 + bias

        top = total = acc = None
        later = score(0)
        for j in range(nj):
            sc = later
            if j + 1 < nj:
                later = score(j + 1)
            peak = rounded(jnp.maximum(jnp.max(sc, axis=1, keepdims=True), FLOOR if top is None else top))
            w = jnp.exp2(sc - peak)
            part = jnp.sum(w, axis=1, keepdims=True)
            val = lax.dot_general(w.astype(BF), keys[:LATENT, j * wj:(j + 1) * wj],
                                  (((1,), (1,)), ((), ())), preferred_element_type=F32)
            if top is None:
                total, acc = part, val
            else:
                scale = jnp.exp2(top - peak)
                total = total * scale + part
                acc = acc * scale + val
            top = peak
        hi = rounded(total)
        lo = total - hi
        for i, (p, t, a) in enumerate(groups):
            for b in range(4):
                store(obuf.at[p, t, a], TILE[b], acc[64 * i + ROWS * b:64 * i + ROWS * b + ROWS])
            tile = jnp.zeros((ROWS, 128), F32)
            for b in range(4):
                part = slice((i * 4 + b) * ROWS, (i * 4 + b + 1) * ROWS)
                tile = jnp.where(lane == b, top[part], tile)
                tile = jnp.where(lane == 4 + b, hi[part], tile)
                tile = jnp.where(lane == 8 + b, lo[part], tile)
            obuf[p, t, a, STAT] = tile.astype(BF)

    def rsem(p, t, i):
        n = (p * NPART + t) * 4 + i
        return rsend.at[n], rrecv.at[n]

    def a1(p, t, sign):
        i = 0 if sign > 0 else 1
        return rdma(obuf.at[p, t, 2, pl.ds(8 * i, 9)], ra.at[p, t, i], *rsem(p, t, i), nbr(p, t, sign))

    def a2(p, t, sign):
        i = 0 if sign > 0 else 1
        return rdma(obuf.at[p, t, 1 if sign > 0 else 3], rc.at[p, t, i], *rsem(p, t, 2 + i), nbr(p, t, sign))

    def back(p, t, d):
        dz, dx = line(p, t, d)
        if t < 3:
            i = t * 7 + (d - 1 if p == 0 else 3 + d)
            if (p, t) in middle and d == 0:
                return rdma(by.at[t], rd.at[i], dsend.at[i], drecv.at[i], (g, other))
            home = y if p == 0 or (p, t) in middle else 1 - y
            return rdma(bb.at[p, t, d], rd.at[i], dsend.at[i], drecv.at[i], (g, at(dz, dx, home)))
        s = (t - 3) * 2 + p
        i = (2 * h + y) * 4 + d
        return rdma(bb.at[p, t, d], rf.at[i], fsend.at[s * 4 + d], frecv.at[i], (s, at(dz, dx, k)))

    def only(pair, keep):
        return jnp.where(keep, pair[0], 4 * FLOOR), jnp.where(keep, pair[1], 0.0)

    def shifted(pair, b):
        if b == 0:
            return pair
        return pltpu.roll(pair[0], 128 - b, 1), pltpu.roll(pair[1], 128 - b, 1)

    def begin(p, t):
        a1(p, t, 1).start()
        a1(p, t, -1).start()

    def r1(units):
        for p, t in units:
            a1(p, t, 1).wait_recv()
            a1(p, t, -1).wait_recv()
        for p, t in units:
            for i in range(2):
                own = obuf.at[p, t, 1 if i == 0 else 3]
                came = ra.at[p, t, i]
                inside = (lane < 2) if i == 0 else (lane >= 2) & (lane < 4)
                top, total, (f0, f1) = combine([stats(own[STAT]), only(stats(came[STAT if i == 0 else 0]), inside)])
                for b in (2 * i, 2 * i + 1):
                    o = load(own, TILE[b]) * f0[:, b:b + 1] + load(came, TILE[b] - 8 * i) * f1[:, b:b + 1]
                    store(own, TILE[b], o)
                own[STAT] = packed(top, total)
        for p, t in units:
            a2(p, t, 1).start()
            a2(p, t, -1).start()

    def r2(units):
        for p, t in units:
            a2(p, t, 1).wait_recv()
            a2(p, t, -1).wait_recv()
        for p, t in units:
            refs = [obuf.at[p, t, 0], rc.at[p, t, 0], rc.at[p, t, 1]]
            top, total, fs = combine([stats(r[STAT]) for r in refs])
            tile = packed(top, total)
            for b in range(4):
                o = load(refs[0], TILE[b]) * fs[0][:, b:b + 1]
                for r, f in zip(refs[1:], fs[1:]):
                    o = o + load(r, TILE[b]) * f[:, b:b + 1]
                store(bb.at[p, t, b], 0, o)
                bb[p, t, b, 4] = tile
        for p, t in units:
            for d in (2, 1, 3):
                back(p, t, d).start()
            if (p, t) in late[:1]:
                back(p, t, 0).start()
            if t >= 3:
                mine = (g == (t - 3) * 2 + p) & (y == k)
                pl.when(jnp.logical_not(mine))(back(p, t, 0).start)

                @pl.when(mine)
                def _():
                    rf[(2 * h + y) * 4] = bb[p, t, 0]

    def r3(units):
        for p, t in units:
            for d in (1, 2, 3):
                back(p, t, d).wait_recv()
        for p, t in units:
            refs = [rd.at[t * 7 + 3 + d] for d in (1, 2, 3)]
            top, total, fs = combine([stats(bb[p, t, 0, 4])] + [shifted(stats(r[4]), d + 1) for d, r in enumerate(refs)])
            o = load(bb.at[p, t, 0], 0) * fs[0][:, 0:1]
            for r, f in zip(refs, fs[1:]):
                o = o + load(r, 0) * f[:, 0:1]
            store(by.at[t], 0, o)
            by[t, 4] = packed(top, total)
        for p, t in units:
            back(p, t, 0).start()

    att = [None] * 4

    def fold_in(t, parts, outs, last):
        parts = parts + [(fst[t, 0], fst[t, 1])]
        top, total, fs = combine(parts)
        o = fo[t] * fs[-1][:, 0:1]
        for f, v in zip(fs[:-1], outs):
            o = o + load(v, 0) * f[:, 0:1]
        if last:
            att[t] = (o / total[:, 0:1]).astype(BF)
        else:
            fo[t] = o
            fst[t, 0] = top
            fst[t, 1] = total

    def fin_half(p, t):
        ds = (1, 2, 3) if p == 0 else (0,) if (p, t) in middle else (0, 1, 2, 3)
        for d in ds:
            back(p, t, d).wait_recv()
        where = [t * 7 + (d - 1 if p == 0 else 3 + d) for d in ds]
        parts = [shifted(stats(rd[i, 4]), d) for i, d in zip(where, ds)]
        outs = [rd.at[i] for i in where]
        if p == 0:
            parts.append(stats(bb[0, t, 0, 4]))
            outs.append(bb.at[0, t, 0])
        fold_in(t, parts, outs, p == 1)

    def fin_slot():
        for i in range(16):
            cp = rdma(bb.at[0, 3, 0], rf.at[i], fsend.at[0], frecv.at[i], (g, c))
            if i % 4 == 0:
                mine = (y == k) & (i // 4 == 2 * h + y)
                pl.when(jnp.logical_not(mine))(cp.wait_recv)
            else:
                cp.wait_recv()
        fold_in(3, [shifted(stats(rf[i, 4]), i % 4) for i in range(16)], [rf.at[i] for i in range(16)], True)

    def each(f, units):
        for u in units:
            f(*u)

    def of(units, *dists):
        return [(p, t, a) for a in dists for p, t in units]

    phase("g1")
    each(send2, early)
    spread(*late[0])
    each(spread, slot_u)
    own_copy.wait()
    phase("B1")
    attend(of(early, 0))
    phase("g2")
    each(relay2, early)
    each(send2, late)
    swap.start()
    phase("B2")
    attend(of(early, 1, 3))
    phase("g3")
    each(send2, slot_u)
    each(ready, early)
    phase("g3y")
    yready(0)
    phase("B3")
    attend(of(early, 2) + of(middle, 0))
    each(begin, early)
    phase("g4")
    each(relay2, late)
    each(relay2, slot_u[:2])
    phase("g4y")
    yready(1, 3)
    phase("B4")
    attend(of(middle, 1, 3))
    phase("g5")
    each(relay2, slot_u[2:])
    swap.wait()

    def slot(i):
        phase("ws%d" % i)
        ready(*slot_u[i])
        phase("S%d" % i)
        attend(of(slot_u[i:i + 1], 0, 1, 2, 3))
        begin(*slot_u[i])
        phase("rs%d" % i)

    slot(0)
    r1(early)
    phase("g6")
    yready(2)
    each(ready, late)
    phase("B5")
    attend(of(middle, 2) + of(late, 2))
    each(begin, middle)
    each(begin, late)
    slot(1)
    slot(2)
    r1(middle)
    r1(slot_u[0:1])
    slot(3)
    r1(slot_u[1:2])
    phase("M3")
    attend(of(late, 1, 3))
    phase("rm3")
    r1(late)
    r1(slot_u[2:3])
    r2(middle)
    phase("E")
    attend(of(late, 0))
    phase("re")
    r1(slot_u[3:])
    r2(slot_u[0:2])
    phase("rlate")
    r2(late)
    phase("rmid")
    r3(middle)
    r2(early)
    phase("rs12")
    r2(slot_u[2:3])
    phase("rs13")
    r2(slot_u[3:])
    phase("f0")
    fin_half(0, 0)
    fin_half(0, 1)
    phase("f1")
    fin_half(0, 2)
    fin_half(1, 0)
    fin_half(1, 1)
    phase("f2")
    fin_half(1, 2)
    phase("fs")
    fin_slot()

    phase("tail")
    attended = jnp.concatenate(att, axis=0)
    vu_copy.wait()
    op_copy.wait()
    row_head = lax.broadcasted_iota(jnp.int32, (64, 128), 0) % 4
    pieces = []
    for head in range(4):
        hv = jnp.dot(attended, vuv[head], preferred_element_type=F32)
        pieces.append(jnp.where(row_head == head, hv, 0.0).astype(BF))
    spread = jnp.concatenate(pieces, axis=1)
    pick = (lax.broadcasted_iota(jnp.int32, (ROWS, 64), 1) // 4
            == lax.broadcasted_iota(jnp.int32, (ROWS, 64), 0))
    joined = jnp.dot(jnp.where(pick, 1.0, 0.0).astype(BF), spread, preferred_element_type=F32).astype(BF)

    def outc(dest, rel):
        return rdma(sbuf.at[dest], rbuf.at[rel], xsend.at[dest], xrecv.at[rel], (g, dest))

    width = 8 * OUTW
    for step in (2, 1, 3, 0):
        blk = (z + step) % 4
        cols = pl.ds(pl.multiple_of(blk * width, 128), width)
        term = jnp.dot(joined, opv[:, cols], preferred_element_type=F32)
        for i in range(8):
            sbuf[blk * 8 + i, :, :OUTW] = term[:, i * OUTW:(i + 1) * OUTW].astype(BF)
        for i in range(8):
            dest = blk * 8 + i
            cp = outc(dest, (c - dest + NPEER) % NPEER)
            if step:
                cp.start()
            else:
                pl.when(dest != c)(cp.start)
    phase("outx")

    handed_do(False)
    for p, t in order:
        for d in (1, 2, 3):
            if (p, t) not in middle:
                along(p, t, d).wait_send()
            back(p, t, d).wait_send()
        if t >= 3:
            mine = (g == (t - 3) * 2 + p) & (y == k)
            pl.when(jnp.logical_not(mine))(back(p, t, 0).wait_send)
        elif p == 1:
            back(p, t, 0).wait_send()
            if (p, t) in middle:
                for a in range(4):
                    yget(t, a).wait_send()
            else:
                across(t).wait_send()
        for sign in (1, -1):
            if (p, t) not in middle:
                g2(p, t, sign).wait_send()
                g2f(p, t, sign).wait_send()
            a1(p, t, sign).wait_send()
            a2(p, t, sign).wait_send()

    res = sbuf[c][:, :OUTW].astype(F32)
    for rel in range(1, NPEER):
        pltpu.make_async_remote_copy(src_ref=sbuf.at[0], dst_ref=rbuf.at[rel], send_sem=xsend.at[0],
                                     recv_sem=xrecv.at[rel], device_id=(g, c), device_id_type=MESH).wait_recv()
        res = res + rbuf[rel][:, :OUTW].astype(F32)
    for t in range(4):
        out_ref[t, 0] = res[4 * t:4 * t + 4].astype(BF)

    def sent_out(i, carry):
        outc((c + i) % NPEER, (NPEER - i) % NPEER).wait_send()
        return carry

    lax.fori_loop(1, NPEER, sent_out, 0)
    phase(None)


def body(cache, queries, new_latent, lengths, donor, value_up, out_proj):
    keys = jnp.swapaxes(cache[0], 0, 1)
    VM, SM, ANY = pltpu.VMEM, pltpu.SMEM, pl.ANY
    U = (2, NPART)
    dma = pltpu.SemaphoreType.DMA
    return pl.pallas_call(
        kernel,
        out_shape=jax.ShapeDtypeStruct((4, 1, 4, OUTW), BF),
        in_specs=[pl.BlockSpec(memory_space=m) for m in (SM, SM, VM, VM, ANY, ANY, ANY)],
        out_specs=pl.BlockSpec(memory_space=VM),
        scratch_shapes=[
            VM((2, KEYW, CTX), BF),
            VM((4, ROWS, KEYW), BF),
            VM(U + (4, 4, ROWS, KEYW), BF),
            VM(U + (4, 17, ROWS, 128), BF),
            VM(U + (2, 9, ROWS, 128), BF),
            VM(U + (2, 17, ROWS, 128), BF),
            VM(U + (4, 5, ROWS, 128), BF),
            VM((2, 5, ROWS, 128), BF),
            VM((21, 5, ROWS, 128), BF),
            VM((16, 5, ROWS, 128), BF),
            VM((NPEER, ROWS, 256), BF), VM((NPEER, ROWS, 256), BF),
            VM((512, 7168), BF), VM((4, LATENT, 128), BF),
            VM((4, ROWS, LATENT), F32), VM((4, 2, ROWS, 128), F32),
            dma((5,)), dma((44,)), dma((40,)), dma((40,)), dma((40,)), dma((40,)), dma((40,)),
            dma((NPEER,)), dma((NPEER,)), dma((21,)), dma((21,)), dma((16,)), dma((16,)),
        ],
        compiler_params=pltpu.CompilerParams(collective_id=0, has_side_effects=True,
                                             vmem_limit_bytes=56 * 1024 * 1024),
        name="mla_step",
    )(lengths, donor, queries, new_latent, keys, value_up, out_proj)


def solution(mesh):
    return jax.shard_map(
        body,
        mesh=mesh,
        in_specs=(
            P("grp", "ctx", None),
            P(None, "grp", None, "ctx", None),
            P(None, "grp", None, None),
            P(),
            P(),
            P("ctx", None, None),
            P("ctx", None),
        ),
        out_specs=P(None, "grp", None, "ctx"),
        check_vma=False,
    )
```
